32 devices in a mesh: elem: 8 (over z, y), bucket: 4 (over x, core).
Axes of the slice: x: 2, y: 2, z: 4, core: 2. Of those that a mesh axis runs over, the one named last changes fastest.
Arguments:
- node_data: float32 [24, 98304], P(None, 'elem'), may hold values from -6 to 6
- eroded: int32 [4096], P('elem'), may hold values from 0 to 2047, as said below
- bucket_map: int32 [98304], P('elem'), may hold values from 0 to 63, as said below
- seg_point: float32 [64, 3, 512], P('elem', None, 'bucket'), may hold values from -3 to 3
- seg_angle: float32 [64, 2, 512], P('elem', None, 'bucket'), may hold values from -3.140625 to 3.140625
Outputs:
- face_force: float32 [3, 24576], P(None, 'elem')
The draws below stay inside these ranges and needn't reach their ends.
Inputs may be any that keep to these rules, and one draw needn't show every extreme that they name: `eroded`: the 512 entries of one index of elem are distinct local element numbers. `bucket_map`: among the faces of the elements listed in eroded, those of one index of elem name one bucket at most 80 times; in every draw some bucket is named exactly 80 times by every index of elem.
All inputs are finite; a program needn't handle non-finite values.
Results may differ from the reference program's by a relative error of at most 0.00012.
Values sent between devices are 32-bit elements; how exact they have to be, the bound alone decides.
No kernel may reach another device: no remote copies, remote signals or barrier semaphores. Data moves between devices by JAX's collectives and lax.ppermute only.
A program may use at most 64 MiB of HBM per device.

```python
import jax
import jax.numpy as jnp
from jax import lax

ELEM_DEV = 2048
ERODE_DEV = 512
SLOT = 80
BUCKETS = 64
SEGS = 512
FACES = 98304
UNCOVERED = 24576
N_ELEM = 8


def erosion_plan(key):
    plan_key = jax.random.fold_in(key, 11)
    elem_key, pool_key, hot_key, fill_key = jax.random.split(plan_key, 4)
    elem_iota = jnp.arange(ELEM_DEV, dtype=jnp.int32)
    elem_scores = jax.random.randint(elem_key, (N_ELEM, ELEM_DEV), 0, 65536, dtype=jnp.int32) * ELEM_DEV + elem_iota[None, :]
    eroded = jnp.argsort(elem_scores, axis=1)[:, :ERODE_DEV].astype(jnp.int32)
    pool_size = BUCKETS * SLOT
    pool_iota = jnp.arange(pool_size, dtype=jnp.int32)
    pool_ids = pool_iota // SLOT
    hot_bucket = jax.random.randint(hot_key, (), 0, BUCKETS, dtype=jnp.int32)
    scores = jax.random.randint(pool_key, (N_ELEM, pool_size), 0, 65536, dtype=jnp.int32) * pool_size + pool_iota[None, :]
    scores = jnp.where((pool_ids == hot_bucket)[None, :], pool_iota[None, :] - pool_size, scores)
    pool_order = jnp.argsort(scores, axis=1)[:, :6 * ERODE_DEV]
    chosen = pool_ids[pool_order].astype(jnp.int32)
    background = jax.random.randint(fill_key, (N_ELEM, 6 * ELEM_DEV), 0, BUCKETS, dtype=jnp.int32)
    sides = jnp.arange(6, dtype=jnp.int32)
    face_index = (6 * eroded[:, :, None] + sides[None, None, :]).reshape(N_ELEM, 6 * ERODE_DEV)
    device_rows = jnp.broadcast_to(jnp.arange(N_ELEM, dtype=jnp.int32)[:, None], face_index.shape)
    bucket_map = background.at[device_rows, face_index].set(chosen)
    return (eroded.reshape(-1), bucket_map.reshape(-1))


def draw_eroded(key, part):
    return erosion_plan(key)[0]


def draw_bucket_map(key, part):
    return erosion_plan(key)[1]


def level_of(stream_key, dims, cuts, least, top_value):
    level = 1.0
    for axis_at, shards_of in cuts:
        heights = jax.random.uniform(jax.random.fold_in(jax.random.fold_in(stream_key, 6), axis_at), (shards_of,), jnp.float32, least / len(cuts), top_value / len(cuts))
        level = level * jnp.repeat(jnp.exp(heights), dims[axis_at] // shards_of).reshape((-1,) + (1,) * (len(dims) - 1 - axis_at))
    return level


def normal_values(own_key, shape, deviation, most, shards=(), held_as=jnp.bfloat16):
    factor_of = level_of(own_key, shape, shards, -0.22, 0.18) if shards else 1.0
    entries = jax.random.normal(own_key, shape, jnp.float32) * deviation * factor_of
    return jnp.minimum(jnp.maximum(entries, -most), most).astype(held_as)


def setup_inputs(seed: int = 0) -> dict:
    key_list = jax.random.split(jax.random.key(seed), 6)
    node_data = normal_values(key_list[0], (24, FACES), 1.0, 6.0, ((1, 8),), jnp.float32)
    eroded = draw_eroded(jax.random.fold_in(key_list[5], 71), 0)
    bucket_map = draw_bucket_map(jax.random.fold_in(key_list[5], 71), 0)
    seg_point = normal_values(key_list[3], (BUCKETS, 3, SEGS), 0.5, 3.0, ((0, 8), (2, 4)), jnp.float32)
    seg_angle = jnp.clip(jax.random.uniform(key_list[4], (BUCKETS, 2, SEGS), jnp.float32, -3.140625, 3.140625), -3.140625, 3.140625)
    return dict(node_data=node_data, eroded=eroded, bucket_map=bucket_map, seg_point=seg_point, seg_angle=seg_angle)


STIFFNESS = 20.0
DAMPING = 0.5

def face_geometry(payload):
    corner = payload[0:12].reshape(4, 3, -1)
    motion = payload[12:24].reshape(4, 3, -1)
    centroid = 0.25 * (corner[0] + corner[1] + corner[2] + corner[3])
    first_edge = corner[2] - corner[0]
    second_edge = corner[3] - corner[1]
    area_x = 0.5 * (first_edge[1] * second_edge[2] - first_edge[2] * second_edge[1])
    area_y = 0.5 * (first_edge[2] * second_edge[0] - first_edge[0] * second_edge[2])
    area_z = 0.5 * (first_edge[0] * second_edge[1] - first_edge[1] * second_edge[0])
    velocity = 0.25 * (motion[0] + motion[1] + motion[2] + motion[3])
    return jnp.concatenate([centroid, jnp.stack([area_x, area_y, area_z]), velocity], axis=0)

def unit_normal(angles):
    return jnp.stack([jnp.cos(angles[:, 0]) * jnp.sin(angles[:, 1]), jnp.sin(angles[:, 0]) * jnp.sin(angles[:, 1]), jnp.cos(angles[:, 1])], axis=1)

def penalty_terms(geometry, point, normal, stiff):
    offset = geometry[0:3, :, None] - point
    dist_sq = offset[0] * offset[0] + offset[1] * offset[1] + offset[2] * offset[2]
    gap_value = offset[0] * normal[0] + offset[1] * normal[1] + offset[2] * normal[2]
    closing = geometry[6][:, None] * normal[0] + geometry[7][:, None] * normal[1] + geometry[8][:, None] * normal[2]
    projected = jnp.abs(geometry[3][:, None] * normal[0] + geometry[4][:, None] * normal[1] + geometry[5][:, None] * normal[2])
    depth_in = jnp.maximum(-gap_value, 0.0)
    weight = jnp.exp(-0.5 * dist_sq)
    return weight * depth_in * (stiff - DAMPING * closing) * projected

def reference(node_data, eroded, bucket_map, seg_point, seg_angle):
    local = eroded.reshape(N_ELEM, ERODE_DEV)
    sides = jnp.arange(6, dtype=jnp.int32)
    face_local = (6 * local[:, :, None] + sides[None, None, :]).reshape(N_ELEM, 6 * ERODE_DEV)
    offsets = (jnp.arange(N_ELEM, dtype=jnp.int32) * (6 * ELEM_DEV)).astype(jnp.int32)
    face_global = (face_local + offsets[:, None]).reshape(-1).astype(jnp.int32)
    bucket = bucket_map[face_global]
    geometry = face_geometry(node_data[:, face_global])
    counts = jnp.zeros((BUCKETS,), jnp.float32).at[bucket].add(1.0)
    stiffness = STIFFNESS * lax.rsqrt(jnp.maximum(counts, 1.0))
    normal_all = unit_normal(seg_angle)
    block_count = UNCOVERED // 128
    geo_blocks = geometry.reshape(9, block_count, 128).transpose(1, 0, 2)
    id_blocks = bucket.reshape(block_count, 128)

    def block_force(items):
        geo, block_ids = items
        point = seg_point[block_ids].transpose(1, 0, 2)
        normal = normal_all[block_ids].transpose(1, 0, 2)
        stiff = stiffness[block_ids][:, None]
        traction = penalty_terms(geo, point, normal, stiff)
        return lax.optimization_barrier(jnp.sum(traction[None, :, :] * normal, axis=2))
    forces = lax.map(block_force, (geo_blocks, id_blocks))
    return forces.transpose(1, 0, 2).reshape(3, UNCOVERED)
```

```python
import functools
import math

import jax
import jax.numpy as jnp
from jax import lax
from jax.experimental import pallas as pl
from jax.experimental.pallas import tpu as pltpu
from jax.sharding import PartitionSpec as P

STIFFNESS = 20.0
DAMPING = 0.5
LANES = 128
SIDES = 6
KAPPA = math.sqrt(0.5 / math.log(2.0))


VMEM = pl.BlockSpec(memory_space=pltpu.VMEM)


def lane_take(table, index):
    return jnp.take_along_axis(table, index, axis=1, mode="promise_in_bounds")


def round_up(n, k):
    return (n + k - 1) // k * k


def index_kernel(buckets, eroded_ref, map_ref, point_ref, angle_ref, pay_ref, bucket_ref, row_ref, lane_ref):
    groups = eroded_ref.shape[0]
    eroded = eroded_ref[...]
    lane = lax.broadcasted_iota(jnp.int32, (groups, LANES), 1)
    for part in range(SIDES):
        at = part * LANES + lane
        face = SIDES * lane_take(eroded, at // SIDES) + at % SIDES
        row_ref[pl.ds(part, groups, stride=SIDES), :] = face // LANES
        lane_ref[pl.ds(part, groups, stride=SIDES), :] = face % LANES
    tiles = groups * SIDES
    map_rows = map_ref.shape[0]
    sub = lax.broadcasted_iota(jnp.int32, (8, LANES), 0)
    bucket_iota = lax.broadcasted_iota(jnp.int32, (round_up(buckets, LANES), LANES), 0)

    def tile(t, hist):
        at_lane = jnp.broadcast_to(lane_ref[pl.ds(t, 1), :], (8, LANES))
        at_row = jnp.broadcast_to(row_ref[pl.ds(t, 1), :], (8, LANES)) - sub
        found = jnp.zeros((8, LANES), jnp.int32)
        for r in range(0, map_rows, 8):
            found = jnp.where(at_row == r, lane_take(map_ref[r : r + 8, :], at_lane), found)
        bucket = jnp.sum(found, axis=0, keepdims=True)
        bucket_ref[pl.ds(t, 1), :] = bucket
        return hist + jnp.where(bucket_iota == bucket, 1.0, 0.0)

    hist = lax.fori_loop(0, tiles, tile, jnp.zeros(bucket_iota.shape, jnp.float32), unroll=4)
    local = point_ref.shape[0]
    for c in range(3):
        pay_ref[c * local : (c + 1) * local, :] = point_ref[:, c, :]
    for c in range(2):
        pay_ref[(3 + c) * local : (4 + c) * local, :] = angle_ref[:, c, :]
    for k in range(bucket_iota.shape[0] // LANES):
        block = hist[k * LANES : (k + 1) * LANES, :]
        pay_ref[5 * local + k : 5 * local + k + 1, :] = jnp.sum(block.T, axis=0, keepdims=True)


def face_kernel(node_ref, row_ref, lane_ref, geo_ref, dense_ref):
    map_rows = dense_ref.shape[1]
    tiles = row_ref.shape[0]

    def dense(g, carry):
        rows = []
        for k in range(24):
            start = (k // 8) * (map_rows * 8) + g * 64 + k % 8
            rows.append(node_ref[pl.ds(start, 8, stride=8), :])
        corner = [rows[3 * k : 3 * k + 3] for k in range(4)]
        motion = [rows[12 + 3 * k : 15 + 3 * k] for k in range(4)]
        at = pl.ds(pl.multiple_of(g * 8, 8), 8)
        first = [corner[2][c] - corner[0][c] for c in range(3)]
        second = [corner[3][c] - corner[1][c] for c in range(3)]
        for c in range(3):
            u, v = (c + 1) % 3, (c + 2) % 3
            total = ((corner[0][c] + corner[1][c]) + corner[2][c]) + corner[3][c]
            dense_ref[c, at, :] = (0.25 * KAPPA) * total
            dense_ref[3 + c, at, :] = (0.5 / KAPPA) * (first[u] * second[v] - first[v] * second[u])
            total = ((motion[0][c] + motion[1][c]) + motion[2][c]) + motion[3][c]
            dense_ref[6 + c, at, :] = (0.25 * DAMPING) * total
        return carry

    lax.fori_loop(0, map_rows // 8, dense, 0, unroll=2)
    sub = lax.broadcasted_iota(jnp.int32, (8, LANES), 0)

    def tile(t, carry):
        at_lane = jnp.broadcast_to(lane_ref[pl.ds(t, 1), :], (8, LANES))
        at_row = jnp.broadcast_to(row_ref[pl.ds(t, 1), :], (8, LANES)) - sub
        found = [jnp.zeros((8, LANES), jnp.float32)] * 9
        for r in range(0, map_rows, 8):
            here = at_row == r
            for q in range(9):
                found[q] = jnp.where(here, lane_take(dense_ref[q, r : r + 8, :], at_lane), found[q])
        for q in range(9):
            geo_ref[q, pl.ds(t, 1), :] = jnp.sum(found[q], axis=0, keepdims=True)
        return carry

    lax.fori_loop(0, tiles, tile, 0, unroll=2)


def force_kernel(local, segs, table_ref, bucket_ref, geo_ref, force_ref, px_ref, stiff_ref):
    blocks, rows = table_ref.shape[0], table_ref.shape[1]
    buckets = blocks * local
    tiles = bucket_ref.shape[0]
    me = lax.axis_index("elem")
    turn = me * local
    wide = px_ref.shape[2]
    per_tile = min(LANES // local, blocks)
    for k in range(wide // LANES):
        group = table_ref[k * per_tile : (k + 1) * per_tile]
        pieces = [group[:, c * local : (c + 1) * local, :].reshape(per_tile * local, segs) for c in range(5)]
        azimuth, polar = pieces[3], pieces[4]
        ring = jnp.sin(polar)
        columns = [KAPPA * pieces[0], KAPPA * pieces[1], KAPPA * pieces[2]]
        columns += [jnp.cos(azimuth) * ring, jnp.sin(azimuth) * ring, jnp.cos(polar)]
        for q in range(6):
            px_ref[q, :, k * LANES : k * LANES + per_tile * local] = columns[q].T
        count = jnp.zeros((1, LANES), jnp.float32)
        for i in range(blocks):
            count = count + table_ref[i, 5 * local + k : 5 * local + k + 1, :]
        stiff_ref[k : k + 1, :] = STIFFNESS * lax.rsqrt(jnp.maximum(count, 1.0))

    def pick(read, at_tile, at_lane):
        value = lane_take(read(0), at_lane)
        for k in range(1, wide // LANES):
            value = jnp.where(at_tile == k, lane_take(read(k), at_lane), value)
        return value

    def tile(t, carry):
        bucket = jnp.broadcast_to(bucket_ref[pl.ds(t, 1), :], (8, LANES))
        spot = bucket ^ turn
        stiff = pick(
            lambda k: jnp.broadcast_to(stiff_ref[k : k + 1, :], (8, LANES)), bucket // LANES, bucket % LANES
        )
        at_tile, at_lane = spot // LANES, spot % LANES
        face = [jnp.broadcast_to(geo_ref[q, pl.ds(t, 1), :], (8, LANES)) for q in range(9)]
        total = [jnp.zeros((8, LANES), jnp.float32)] * 3
        for s in range(0, segs, 8):
            p = [
                pick(lambda k: px_ref[q, s : s + 8, k * LANES : (k + 1) * LANES], at_tile, at_lane)
                for q in range(6)
            ]
            m = p[3:]
            d = [face[c] - p[c] for c in range(3)]
            dist = d[0] * d[0] + d[1] * d[1] + d[2] * d[2]
            gap = d[0] * m[0] + d[1] * m[1] + d[2] * m[2]
            area = face[3] * m[0] + face[4] * m[1] + face[5] * m[2]
            closing = face[6] * m[0] + face[7] * m[1] + face[8] * m[2]
            traction = (
                (jnp.exp2(-dist) * jnp.maximum(-gap, 0.0)) * (stiff - closing) * jnp.abs(area)
            )
            total = [total[c] + traction * m[c] for c in range(3)]
        for c in range(3):
            force_ref[c, pl.ds(t, 1), :] = jnp.sum(total[c], axis=0, keepdims=True)
        return carry

    lax.fori_loop(0, tiles, tile, 0, unroll=2)


def swap(value, axis, mask):
    size = lax.axis_size(axis)
    return lax.ppermute(value, axis, [(i, i ^ mask) for i in range(size)])


def local(node_data, eroded, bucket_map, seg_point, seg_angle):
    elem_count = lax.axis_size("elem")
    bucket_split = lax.axis_size("bucket")
    held, _, segs = seg_point.shape
    buckets = held * elem_count
    erode_count = eroded.shape[0]
    faces = node_data.shape[1]
    tiles = SIDES * erode_count // LANES
    map_rows = faces // LANES
    wide = round_up(buckets, LANES)
    pay_rows = round_up(5 * held + wide // LANES, 8)

    pay, face_bucket, face_row, face_lane = pl.pallas_call(
        functools.partial(index_kernel, buckets),
        out_shape=(
            jax.ShapeDtypeStruct((pay_rows, LANES), jnp.float32),
            jax.ShapeDtypeStruct((tiles, LANES), jnp.int32),
            jax.ShapeDtypeStruct((tiles, LANES), jnp.int32),
            jax.ShapeDtypeStruct((tiles, LANES), jnp.int32),
        ),
        in_specs=[VMEM] * 4,
        out_specs=[VMEM] * 4,
        name="index",
        cost_estimate=pl.CostEstimate(flops=4_000_000, bytes_accessed=100_000, transcendentals=0),
    )(eroded.reshape(-1, LANES), bucket_map.reshape(-1, LANES), seg_point, seg_angle)

    gathered = pay[None]
    bit = 1
    while bit < elem_count:
        masks = (bit, 2 * bit, 3 * bit) if 2 * bit < elem_count else (bit,)
        gathered = jnp.concatenate([gathered] + [swap(gathered, "elem", m) for m in masks], axis=0)
        bit *= len(masks) + 1

    nodes = node_data.reshape(3, 8, map_rows, LANES).transpose(0, 2, 1, 3).reshape(24 * map_rows, LANES)
    geometry = pl.pallas_call(
        face_kernel,
        out_shape=jax.ShapeDtypeStruct((9, tiles, LANES), jnp.float32),
        in_specs=[VMEM] * 3,
        out_specs=VMEM,
        scratch_shapes=[pltpu.VMEM((9, map_rows, LANES), jnp.float32)],
        name="faces",
        cost_estimate=pl.CostEstimate(flops=8_000_000, bytes_accessed=1_300_000, transcendentals=0),
    )(nodes, face_row, face_lane)

    force = pl.pallas_call(
        functools.partial(force_kernel, held, segs),
        out_shape=jax.ShapeDtypeStruct((3, tiles, LANES), jnp.float32),
        in_specs=[VMEM] * 3,
        out_specs=VMEM,
        scratch_shapes=[
            pltpu.VMEM((6, segs, wide), jnp.float32),
            pltpu.VMEM((round_up(wide // LANES, 8), LANES), jnp.float32),
        ],
        name="forces",
        cost_estimate=pl.CostEstimate(flops=16_000_000, bytes_accessed=400_000, transcendentals=0),
    )(gathered, face_bucket, geometry)

    force = force.reshape(3, tiles * LANES)
    bit = 1
    while bit < bucket_split:
        force = force + swap(force, "bucket", bit)
        bit *= 2
    return force


def solution(mesh):
    in_specs = (
        P(None, "elem"),
        P("elem"),
        P("elem"),
        P("elem", None, "bucket"),
        P("elem", None, "bucket"),
    )
    return jax.shard_map(local, mesh=mesh, in_specs=in_specs, out_specs=P(None, "elem"), check_vma=False)
```

```python
import functools
import math

import jax
import jax.numpy as jnp
from jax import lax
from jax.experimental import pallas as pl
from jax.experimental.pallas import tpu as pltpu
from jax.sharding import PartitionSpec as P

STIFFNESS = 20.0
DAMPING = 0.5
LANES = 128
SIDES = 6
KAPPA = math.sqrt(0.5 / math.log(2.0))


VMEM = pl.BlockSpec(memory_space=pltpu.VMEM)
HBM = pl.BlockSpec(memory_space=pltpu.HBM)


def lane_take(table, index):
    return jnp.take_along_axis(table, index, axis=1, mode="promise_in_bounds")


def round_up(n, k):
    return (n + k - 1) // k * k


def fetch(pairs, sems):
    copies = [pltpu.make_async_copy(source, target, sems.at[k]) for k, (source, target) in enumerate(pairs)]
    for copy in copies:
        copy.start()
    return copies


def index_kernel(buckets, *refs):
    inputs, (pay_ref, bucket_ref, row_ref, lane_ref), (eroded_ref, map_ref, point_ref, angle_ref, sems) = (
        refs[:4],
        refs[4:8],
        refs[8:],
    )
    copies = fetch(zip(inputs, (eroded_ref, map_ref, point_ref, angle_ref)), sems)
    copies[0].wait()
    groups = eroded_ref.shape[0]
    eroded = eroded_ref[...]
    lane = lax.broadcasted_iota(jnp.int32, (groups, LANES), 1)
    for part in range(SIDES):
        at = part * LANES + lane
        face = SIDES * lane_take(eroded, at // SIDES) + at % SIDES
        row_ref[pl.ds(part, groups, stride=SIDES), :] = face // LANES
        lane_ref[pl.ds(part, groups, stride=SIDES), :] = face % LANES
    tiles = groups * SIDES
    map_rows = map_ref.shape[0]
    sub = lax.broadcasted_iota(jnp.int32, (8, LANES), 0)
    bucket_iota = lax.broadcasted_iota(jnp.int32, (buckets, LANES), 0)
    copies[1].wait()

    def tile(t, hist):
        at_lane = jnp.broadcast_to(lane_ref[pl.ds(t, 1), :], (8, LANES))
        at_row = jnp.broadcast_to(row_ref[pl.ds(t, 1), :], (8, LANES)) - sub
        found = jnp.zeros((8, LANES), jnp.int32)
        for r in range(0, map_rows, 8):
            found = jnp.where(at_row == r, lane_take(map_ref[r : r + 8, :], at_lane), found)
        bucket = jnp.sum(found, axis=0, keepdims=True)
        bucket_ref[pl.ds(t, 1), :] = bucket
        return hist + jnp.where(bucket_iota == bucket, 1.0, 0.0)

    hist = lax.fori_loop(0, tiles, tile, jnp.zeros(bucket_iota.shape, jnp.float32), unroll=6)
    local = point_ref.shape[1]
    copies[2].wait()
    for c in range(3):
        pay_ref[c * local : (c + 1) * local, :] = point_ref[c]
    copies[3].wait()
    for c in range(2):
        pay_ref[(3 + c) * local : (4 + c) * local, :] = angle_ref[:, c, :]
    for k in range(0, buckets, LANES):
        block = hist[k : k + LANES, :]
        row = 5 * local + k // LANES
        pay_ref[row : row + 1, 0 : block.shape[0]] = jnp.sum(block.T, axis=0, keepdims=True)


def split(value, parts):
    pieces = []
    for _ in range(parts):
        piece = value.astype(jnp.bfloat16)
        pieces.append(piece)
        value = value - piece.astype(jnp.float32)
    return pieces


def dense_kernel(node_ref, dense_ref):
    map_rows = dense_ref.shape[0] // 9

    def dense(g, carry):
        values = [[] for _ in range(9)]
        for h in range(2):
            rows = []
            for k in range(24):
                start = (k // 8) * (map_rows * 8) + (2 * g + h) * 64 + k % 8
                rows.append(node_ref[pl.ds(start, 8, stride=8), :])
            corner = [rows[3 * k : 3 * k + 3] for k in range(4)]
            motion = [rows[12 + 3 * k : 15 + 3 * k] for k in range(4)]
            first = [corner[2][c] - corner[0][c] for c in range(3)]
            second = [corner[3][c] - corner[1][c] for c in range(3)]
            for c in range(3):
                u, v = (c + 1) % 3, (c + 2) % 3
                total = ((corner[0][c] + corner[1][c]) + corner[2][c]) + corner[3][c]
                values[c].append((0.25 * KAPPA) * total)
                values[3 + c].append((0.5 / KAPPA) * (first[u] * second[v] - first[v] * second[u]))
                total = ((motion[0][c] + motion[1][c]) + motion[2][c]) + motion[3][c]
                values[6 + c].append((0.25 * DAMPING) * total)
        for q in range(9):
            at = pl.ds(pl.multiple_of(q * map_rows + g * 16, 16), 16)
            high, low = split(jnp.concatenate(values[q], axis=0), 2)
            dense_ref[at, 0:LANES] = high
            dense_ref[at, LANES : 2 * LANES] = low
        return carry

    lax.fori_loop(0, map_rows // 16, dense, 0)


def face_kernel(dense_ref, row_ref, lane_ref, geo_ref, corner_ref, found0_ref, found1_ref):
    map_rows = dense_ref.shape[0] // 9
    step = found0_ref.shape[1]
    tiles = row_ref.shape[0]
    per_step = step // LANES
    lane_iota = lax.broadcasted_iota(jnp.int32, (LANES, LANES), 0)
    sub = lax.broadcasted_iota(jnp.int32, (8, LANES), 0)
    corner_ref[...] = jnp.zeros(corner_ref.shape, corner_ref.dtype)

    def gather(i, found_ref):
        hot = []
        for k in range(per_step):
            here = lane_iota == lane_ref[pl.ds(i * per_step + k, 1), :]
            hot.append(jnp.where(here, 1.0, 0.0).astype(jnp.bfloat16))
        hot = jnp.concatenate(hot, axis=1)
        hot = jnp.concatenate([hot, hot], axis=0)
        found_ref[...] = jnp.dot(dense_ref[...], hot, preferred_element_type=jnp.float32)

    def select(i, found_ref):
        for k in range(per_step):
            t = i * per_step + k
            at_row = jnp.broadcast_to(row_ref[pl.ds(t, 1), :], (8, LANES)) - sub
            found = [jnp.zeros((8, LANES), jnp.float32)] * 9
            for r in range(0, map_rows, 8):
                here = at_row == r
                for q in range(9):
                    at = q * map_rows + r
                    found[q] = jnp.where(here, found_ref[at : at + 8, k * LANES : (k + 1) * LANES], found[q])
            for q in range(9):
                geo_ref[t, q : q + 1, :] = jnp.sum(found[q], axis=0, keepdims=True)

    pipelined(tiles // per_step, gather, select, found0_ref, found1_ref)

    def pieces(t, carry):
        corner_ref[t, 0:9, :] = jnp.concatenate(split(geo_ref[t, 0:3, :], 3), axis=0)
        return carry

    lax.fori_loop(0, tiles, pieces, 0, unroll=4)


def pipelined(steps, produce, consume, ref0, ref1):
    produce(0, ref0)

    def body(i, carry):
        produce(2 * i + 1, ref1)
        consume(2 * i, ref0)
        produce(jnp.minimum(2 * i + 2, steps - 1), ref0)
        consume(2 * i + 1, ref1)
        return carry

    lax.fori_loop(0, steps // 2, body, 0)


def table_columns(refs, local):
    rows = [jnp.concatenate([r[c * local : (c + 1) * local, :] for r in refs], axis=0) for c in range(5)]
    azimuth, polar = rows[3], rows[4]
    ring = jnp.sin(polar)
    columns = [KAPPA * rows[0], KAPPA * rows[1], KAPPA * rows[2]]
    return columns + [jnp.cos(azimuth) * ring, jnp.sin(azimuth) * ring, jnp.cos(polar)]


def put_table(table, local, segs, start, hot_ref):
    blocks = table.shape[0]
    group = min(LANES // local, blocks)
    for b0 in range(0, blocks, group):
        columns = table_columns([table.at[b] for b in range(b0, b0 + group)], local)
        for q in range(6):
            for k, piece in enumerate(split(columns[q].T, 3)):
                at = start + k * blocks * local + b0 * local
                for g in range(0, segs, 16):
                    row = 6 * g + 16 * q
                    hot_ref[row : row + 16, at : at + group * local] = piece[g : g + 16]


def table_kernel(local, segs, table_ref, hot_ref):
    put_table(table_ref, local, segs, 0, hot_ref)
    tail = hot_ref.shape[1] - 16
    lane = lax.broadcasted_iota(jnp.int32, (96, 16), 1)
    value = lax.broadcasted_iota(jnp.int32, (96, 16), 0) // 16
    take_off = jnp.where((lane % 3 == value) & (lane < 9), -1.0, 0.0).astype(jnp.bfloat16)
    for g in range(0, segs, 16):
        hot_ref[6 * g : 6 * g + 96, tail : tail + 16] = take_off


def force_kernel(local, segs, tables, refs):
    half_ref, bucket_ref, geo_ref, corner_ref, force_ref, hot_ref, stiff_ref, found0_ref, found1_ref = refs
    per_table = tables[0].shape[0]
    per_table_buckets = per_table * local
    tiles = bucket_ref.shape[0]
    wide = stiff_ref.shape[0] * LANES
    step = found0_ref.shape[1]
    per_step = step // LANES
    turn = lax.axis_index("elem") * local
    hot_ref[...] = half_ref[...]
    for n, table in enumerate(tables[1:]):
        put_table(table, local, segs, (n + 1) * 3 * per_table_buckets, hot_ref)
    for k in range(wide // LANES):
        count = jnp.zeros((1, LANES), jnp.float32)
        for table in tables:
            for b in range(per_table):
                count = count + table[b, 5 * local + k : 5 * local + k + 1, :]
        stiff_ref[k : k + 1, :] = STIFFNESS * lax.rsqrt(jnp.maximum(count, 1.0))
    sub = lax.broadcasted_iota(jnp.int32, (per_table_buckets, LANES), 0)

    def gather(i, found_ref):
        hot = []
        for k in range(per_step):
            t = i * per_step + k
            spot = bucket_ref[pl.ds(t, 1), :] ^ turn
            rows = []
            for n in range(len(tables)):
                here = sub == spot - n * per_table_buckets
                rows += [jnp.where(here, 1.0, 0.0).astype(jnp.bfloat16)] * 3
            hot.append(jnp.concatenate(rows + [corner_ref[t]], axis=0))
        hot = jnp.concatenate(hot, axis=1)
        found_ref[...] = jnp.dot(hot_ref[...], hot, preferred_element_type=jnp.float32)

    def force(i, found_ref):
        for k in range(per_step):
            t = i * per_step + k
            bucket = jnp.broadcast_to(bucket_ref[pl.ds(t, 1), :], (8, LANES))
            stiff = lane_take(jnp.broadcast_to(stiff_ref[0:1, :], (8, LANES)), bucket % LANES)
            for n in range(1, wide // LANES):
                other = lane_take(jnp.broadcast_to(stiff_ref[n : n + 1, :], (8, LANES)), bucket % LANES)
                stiff = jnp.where(bucket // LANES == n, other, stiff)
            face = [jnp.broadcast_to(geo_ref[t, q : q + 1, :], (8, LANES)) for q in range(3, 9)]
            total = [jnp.zeros((8, LANES), jnp.float32)] * 3
            for s in range(0, segs, 8):
                row = s // 16 * 96 + s % 16
                found = [
                    found_ref[row + 16 * q : row + 16 * q + 8, k * LANES : (k + 1) * LANES] for q in range(6)
                ]
                d, m = found[:3], found[3:]
                dist = d[0] * d[0] + d[1] * d[1] + d[2] * d[2]
                depth = d[0] * m[0] + d[1] * m[1] + d[2] * m[2]
                area = face[0] * m[0] + face[1] * m[1] + face[2] * m[2]
                closing = face[3] * m[0] + face[4] * m[1] + face[5] * m[2]
                traction = (jnp.exp2(-dist) * jnp.maximum(depth, 0.0)) * (
                    (stiff - closing) * jnp.abs(area)
                )
                total = [total[c] + traction * m[c] for c in range(3)]
            at = pl.ds(pl.multiple_of(t * LANES, LANES), LANES)
            for c in range(3):
                force_ref[c : c + 1, at] = jnp.sum(total[c], axis=0, keepdims=True)

    pipelined(tiles // per_step, gather, force, found0_ref, found1_ref)


def swap(value, axis, mask):
    size = lax.axis_size(axis)
    return lax.ppermute(value, axis, [(i, i ^ mask) for i in range(size)])


def local(node_data, eroded, bucket_map, seg_point, seg_angle):
    elem_count = lax.axis_size("elem")
    bucket_split = lax.axis_size("bucket")
    held, _, segs = seg_point.shape
    buckets = held * elem_count
    erode_count = eroded.shape[0]
    faces = node_data.shape[1]
    tiles = SIDES * erode_count // LANES
    map_rows = faces // LANES
    wide = round_up(buckets, LANES)
    pay_rows = round_up(5 * held + wide // LANES, 8)
    step = 2 * LANES
    inputs = (eroded.reshape(-1, LANES), bucket_map.reshape(-1, LANES), seg_point.transpose(1, 0, 2), seg_angle)

    pay, face_bucket, face_row, face_lane = pl.pallas_call(
        functools.partial(index_kernel, buckets),
        out_shape=(
            jax.ShapeDtypeStruct((pay_rows, LANES), jnp.float32),
            jax.ShapeDtypeStruct((tiles, LANES), jnp.int32),
            jax.ShapeDtypeStruct((tiles, LANES), jnp.int32),
            jax.ShapeDtypeStruct((tiles, LANES), jnp.int32),
        ),
        in_specs=[HBM] * 4,
        out_specs=[VMEM] * 4,
        scratch_shapes=[pltpu.VMEM(x.shape, x.dtype) for x in inputs] + [pltpu.SemaphoreType.DMA((4,))],
        name="index",
        compiler_params=pltpu.CompilerParams(vmem_limit_bytes=67043328),
        cost_estimate=pl.CostEstimate(flops=4_000_000, bytes_accessed=100_000, transcendentals=0),
    )(*inputs)

    nodes = node_data.reshape(3, 8, map_rows, LANES).transpose(0, 2, 1, 3).reshape(24 * map_rows, LANES)
    dense = pl.pallas_call(
        dense_kernel,
        out_shape=jax.ShapeDtypeStruct((9 * map_rows, 2 * LANES), jnp.bfloat16),
        in_specs=[VMEM],
        out_specs=VMEM,
        name="dense",
        compiler_params=pltpu.CompilerParams(vmem_limit_bytes=16 * 2**20),
        cost_estimate=pl.CostEstimate(flops=4_000_000, bytes_accessed=1_300_000, transcendentals=0),
    )(nodes)

    tables = [pay[None]]
    bit = 1
    while bit < elem_count:
        masks = (bit, 2 * bit, 3 * bit) if 2 * bit < elem_count else (bit,)
        if bit > 1:
            tables, dense = lax.optimization_barrier((tables, dense))
            tables = [jnp.concatenate(tables, axis=0)]
        tables += [swap(tables[0], "elem", m) for m in masks]
        bit *= len(masks) + 1

    geometry, corner = pl.pallas_call(
        face_kernel,
        out_shape=(
            jax.ShapeDtypeStruct((tiles, 16, LANES), jnp.float32),
            jax.ShapeDtypeStruct((tiles, 16, LANES), jnp.bfloat16),
        ),
        in_specs=[VMEM] * 3,
        out_specs=[VMEM] * 2,
        scratch_shapes=[
            pltpu.VMEM((9 * map_rows, step), jnp.float32),
            pltpu.VMEM((9 * map_rows, step), jnp.float32),
        ],
        name="faces",
        compiler_params=pltpu.CompilerParams(vmem_limit_bytes=16 * 2**20),
        cost_estimate=pl.CostEstimate(flops=8_000_000, bytes_accessed=500_000, transcendentals=0),
    )(dense, face_row, face_lane)

    columns = 3 * buckets + 16
    half = pl.pallas_call(
        functools.partial(table_kernel, held, segs),
        out_shape=jax.ShapeDtypeStruct((6 * segs, columns), jnp.bfloat16),
        in_specs=[VMEM],
        out_specs=VMEM,
        name="table",
        compiler_params=pltpu.CompilerParams(vmem_limit_bytes=16 * 2**20),
        cost_estimate=pl.CostEstimate(flops=4_000_000, bytes_accessed=100_000, transcendentals=0),
    )(tables[0])
    force = pl.pallas_call(
        lambda *refs: force_kernel(held, segs, refs[: len(tables)], refs[len(tables) :]),
        out_shape=jax.ShapeDtypeStruct((3, tiles * LANES), jnp.float32),
        in_specs=[VMEM] * (4 + len(tables)),
        out_specs=VMEM,
        scratch_shapes=[
            pltpu.VMEM((6 * segs, columns), jnp.bfloat16),
            pltpu.VMEM((wide // LANES, LANES), jnp.float32),
            pltpu.VMEM((6 * segs, step), jnp.float32),
            pltpu.VMEM((6 * segs, step), jnp.float32),
        ],
        name="forces",
        compiler_params=pltpu.CompilerParams(vmem_limit_bytes=24 * 2**20),
        cost_estimate=pl.CostEstimate(flops=16_000_000, bytes_accessed=400_000, transcendentals=0),
    )(*tables, half, face_bucket, geometry, corner)

    bit = 1
    while bit < bucket_split:
        force = force + swap(force, "bucket", bit)
        bit *= 2
    return force


def solution(mesh):
    in_specs = (
        P(None, "elem"),
        P("elem"),
        P("elem"),
        P("elem", None, "bucket"),
        P("elem", None, "bucket"),
    )
    return jax.shard_map(local, mesh=mesh, in_specs=in_specs, out_specs=P(None, "elem"), check_vma=False)
```

```python
import functools
import math

import jax
import jax.numpy as jnp
from jax import lax
from jax.experimental import pallas as pl
from jax.experimental.pallas import tpu as pltpu
from jax.sharding import PartitionSpec as P

STIFFNESS = 20.0
DAMPING = 0.5
LANES = 128
SIDES = 6
KAPPA = math.sqrt(0.5 / math.log(2.0))


VMEM = pl.BlockSpec(memory_space=pltpu.VMEM)
HBM = pl.BlockSpec(memory_space=pltpu.HBM)


def lane_take(table, index):
    return jnp.take_along_axis(table, index, axis=1, mode="promise_in_bounds")


def round_order(bits):
    return list(range(bits))


def round_up(n, k):
    return (n + k - 1) // k * k


def fetch(pairs, sems):
    copies = [pltpu.make_async_copy(source, target, sems.at[k]) for k, (source, target) in enumerate(pairs)]
    for copy in copies:
        copy.start()
    return copies


def index_kernel(buckets, *refs):
    inputs, (pay_ref, bucket_ref, row_ref, lane_ref) = refs[:4], refs[4:8]
    eroded_ref, map_ref, point_ref, angle_ref, packed_ref, sems = refs[8:]
    copies = fetch(zip(inputs, (eroded_ref, map_ref, point_ref, angle_ref)), sems)
    groups = eroded_ref.shape[0]
    lane = lax.broadcasted_iota(jnp.int32, (groups, LANES), 1)
    ats = [part * LANES + lane for part in range(SIDES)]
    picks = [(at // SIDES, at % SIDES) for at in ats]
    bits = max(1, (buckets - 1).bit_length())
    words = packed_ref.shape[0] // 8
    copies[0].wait()
    eroded = SIDES * eroded_ref[...]
    for part in range(SIDES):
        at, side = picks[part]
        face = lane_take(eroded, at) + side
        row_ref[pl.ds(part, groups, stride=SIDES), :] = face >> 7
        lane_ref[pl.ds(part, groups, stride=SIDES), :] = face & (LANES - 1)
    tiles = groups * SIDES
    map_rows = map_ref.shape[0]
    sub = lax.broadcasted_iota(jnp.int32, (8, LANES), 0)
    bucket_iota = lax.broadcasted_iota(jnp.int32, (buckets, LANES), 0)
    copies[1].wait()
    for w in range(words):
        word = map_ref[8 * w : 8 * w + 8, :]
        for k in range(1, -(-(map_rows // 8 - w) // words)):
            r = 8 * (w + k * words)
            word = word | (map_ref[r : r + 8, :] << (bits * k))
        packed_ref[8 * w : 8 * w + 8, :] = word
    hist = jnp.zeros(bucket_iota.shape, jnp.float32)

    def tile(t, hist):
        at_lane = jnp.broadcast_to(lane_ref[pl.ds(t, 1), :], (8, LANES))
        row = jnp.broadcast_to(row_ref[pl.ds(t, 1), :], (8, LANES))
        group = row >> 3
        slot = sum(((group >= k * words).astype(jnp.int32) for k in range(1, -(-(map_rows // 8) // words))), 0)
        key = ((group - slot * words) << 3) + (row & 7) - sub
        found = jnp.zeros((8, LANES), jnp.int32)
        for w in range(words):
            found = jnp.where(key == 8 * w, lane_take(packed_ref[8 * w : 8 * w + 8, :], at_lane), found)
        found = jnp.sum(found, axis=0, keepdims=True)
        bucket = (found >> (bits * slot[0:1])) & (2**bits - 1)
        bucket_ref[pl.ds(t, 1), :] = bucket
        return hist + jnp.where(bucket_iota == bucket, 1.0, 0.0)

    unroll = tiles if buckets <= LANES else 2
    hist = lax.fori_loop(0, tiles, tile, hist, unroll=unroll)
    local = point_ref.shape[1]
    copies[2].wait()
    for c in range(3):
        pay_ref[c * local : (c + 1) * local, :] = point_ref[c]
    copies[3].wait()
    for c in range(2):
        pay_ref[(3 + c) * local : (4 + c) * local, :] = angle_ref[:, c, :]
    for k in range(0, buckets, LANES):
        block = hist[k : k + LANES, :]
        row = 5 * local + k // LANES
        pay_ref[row : row + 1, 0 : block.shape[0]] = jnp.sum(block.T, axis=0, keepdims=True)


def split(value, parts):
    pieces = []
    for _ in range(parts):
        piece = value.astype(jnp.bfloat16)
        pieces.append(piece)
        value = value - piece.astype(jnp.float32)
    return pieces


def dense_kernel(node_ref, dense_ref):
    map_rows = dense_ref.shape[0] // 9

    def dense(g, carry):
        values = [[] for _ in range(9)]
        for h in range(2):
            rows = []
            for k in range(24):
                start = (k // 8) * (map_rows * 8) + (2 * g + h) * 64 + k % 8
                rows.append(node_ref[pl.ds(start, 8, stride=8), :])
            corner = [rows[3 * k : 3 * k + 3] for k in range(4)]
            motion = [rows[12 + 3 * k : 15 + 3 * k] for k in range(4)]
            first = [corner[2][c] - corner[0][c] for c in range(3)]
            second = [corner[3][c] - corner[1][c] for c in range(3)]
            for c in range(3):
                u, v = (c + 1) % 3, (c + 2) % 3
                total = ((corner[0][c] + corner[1][c]) + corner[2][c]) + corner[3][c]
                values[c].append((0.25 * KAPPA) * total)
                values[3 + c].append((0.5 / KAPPA) * (first[u] * second[v] - first[v] * second[u]))
                total = ((motion[0][c] + motion[1][c]) + motion[2][c]) + motion[3][c]
                values[6 + c].append((0.25 * DAMPING) * total)
        for q in range(9):
            at = pl.ds(pl.multiple_of(q * map_rows + g * 16, 16), 16)
            high, low = split(jnp.concatenate(values[q], axis=0), 2)
            dense_ref[at, 0:LANES] = high
            dense_ref[at, LANES : 2 * LANES] = low
        return carry

    lax.fori_loop(0, map_rows // 16, dense, 0)


def face_kernel(dense_ref, row_ref, lane_ref, geo_ref, corner_ref, found0_ref, found1_ref):
    map_rows = dense_ref.shape[0] // 9
    step = found0_ref.shape[1]
    tiles = row_ref.shape[0]
    per_step = step // LANES
    lane_iota = lax.broadcasted_iota(jnp.int32, (LANES, LANES), 0)
    sub = lax.broadcasted_iota(jnp.int32, (8, LANES), 0)
    corner_ref[...] = jnp.zeros(corner_ref.shape, corner_ref.dtype)

    def gather(i, found_ref):
        hot = []
        for k in range(per_step):
            here = lane_iota == lane_ref[pl.ds(i * per_step + k, 1), :]
            hot.append(jnp.where(here, 1.0, 0.0).astype(jnp.bfloat16))
        hot = jnp.concatenate(hot, axis=1)
        hot = jnp.concatenate([hot, hot], axis=0)
        found_ref[...] = jnp.dot(dense_ref[...], hot, preferred_element_type=jnp.float32)

    def select(i, found_ref):
        for k in range(per_step):
            t = i * per_step + k
            at_row = jnp.broadcast_to(row_ref[pl.ds(t, 1), :], (8, LANES)) - sub
            found = [jnp.zeros((8, LANES), jnp.float32)] * 9
            for r in range(0, map_rows, 8):
                here = at_row == r
                for q in range(9):
                    at = q * map_rows + r
                    found[q] = jnp.where(here, found_ref[at : at + 8, k * LANES : (k + 1) * LANES], found[q])
            for q in range(9):
                geo_ref[t, q : q + 1, :] = jnp.sum(found[q], axis=0, keepdims=True)

    pipelined(tiles // per_step, gather, select, found0_ref, found1_ref)

    def pieces(t, carry):
        corner_ref[t, 0:9, :] = jnp.concatenate(split(geo_ref[t, 0:3, :], 3), axis=0)
        return carry

    lax.fori_loop(0, tiles, pieces, 0, unroll=4)


def pipelined(steps, produce, consume, ref0, ref1):
    refs = (ref0, ref1)
    produce(0, ref0)
    for i in range(steps):
        if i + 1 < steps:
            produce(i + 1, refs[(i + 1) % 2])
        consume(i, refs[i % 2])


def table_columns(refs, local):
    rows = [jnp.concatenate([r[c * local : (c + 1) * local, :] for r in refs], axis=0) for c in range(5)]
    azimuth, polar = rows[3], rows[4]
    ring = jnp.sin(polar)
    columns = [KAPPA * rows[0], KAPPA * rows[1], KAPPA * rows[2]]
    return columns + [jnp.cos(azimuth) * ring, jnp.sin(azimuth) * ring, jnp.cos(polar)]


def put_table(table, local, segs, start, hot_ref):
    blocks = table.shape[0] // (5 * local)
    group = min(LANES // local, blocks)
    for b0 in range(0, blocks, group):
        columns = table_columns([table.at[5 * local * b :] for b in range(b0, b0 + group)], local)
        for q in range(6):
            for k, piece in enumerate(split(columns[q].T, 3)):
                at = start + k * blocks * local + b0 * local
                for g in range(0, segs, 16):
                    row = 6 * g + 16 * q
                    hot_ref[row : row + 16, at : at + group * local] = piece[g : g + 16]


def table_kernel(local, segs, table_ref, hot_ref):
    put_table(table_ref, local, segs, 0, hot_ref)
    tail = hot_ref.shape[1] - 16
    lane = lax.broadcasted_iota(jnp.int32, (96, 16), 1)
    value = lax.broadcasted_iota(jnp.int32, (96, 16), 0) // 16
    take_off = jnp.where((lane % 3 == value) & (lane < 9), -1.0, 0.0).astype(jnp.bfloat16)
    for g in range(0, segs, 16):
        hot_ref[6 * g : 6 * g + 96, tail : tail + 16] = take_off


def force_kernel(local, segs, order, tables, refs):
    half_ref, bucket_ref, geo_ref, corner_ref, force_ref, hot_ref, stiff_ref, found0_ref, found1_ref = refs
    per_table_buckets = tables[0].shape[0] // (5 * local) * local
    count_at = 5 * per_table_buckets
    tiles = bucket_ref.shape[0]
    wide = stiff_ref.shape[0] * LANES
    step = found0_ref.shape[1]
    per_step = step // LANES
    turn = lax.axis_index("elem") * local
    hot_ref[...] = half_ref[...]
    for n, table in enumerate(tables[1:]):
        put_table(table, local, segs, (n + 1) * 3 * per_table_buckets, hot_ref)
    for k in range(wide // LANES):
        count = sum(table[count_at + k : count_at + k + 1, :] for table in tables)
        stiff_ref[k : k + 1, :] = STIFFNESS * lax.rsqrt(jnp.maximum(count, 1.0))
    sub = lax.broadcasted_iota(jnp.int32, (per_table_buckets, LANES), 0)

    def gather(i, found_ref):
        hot = []
        for k in range(per_step):
            t = i * per_step + k
            spot = bucket_ref[pl.ds(t, 1), :] ^ turn
            owner = sum(((spot // local >> bit) & 1) << k for k, bit in enumerate(order))
            spot = owner * local + spot % local
            rows = []
            for n in range(len(tables)):
                here = sub == spot - n * per_table_buckets
                rows += [jnp.where(here, 1.0, 0.0).astype(jnp.bfloat16)] * 3
            hot.append(jnp.concatenate(rows + [corner_ref[t]], axis=0))
        hot = jnp.concatenate(hot, axis=1)
        found_ref[...] = jnp.dot(hot_ref[...], hot, preferred_element_type=jnp.float32)

    def force(i, found_ref):
        for k in range(per_step):
            t = i * per_step + k
            bucket = jnp.broadcast_to(bucket_ref[pl.ds(t, 1), :], (8, LANES))
            stiff = lane_take(jnp.broadcast_to(stiff_ref[0:1, :], (8, LANES)), bucket % LANES)
            for n in range(1, wide // LANES):
                other = lane_take(jnp.broadcast_to(stiff_ref[n : n + 1, :], (8, LANES)), bucket % LANES)
                stiff = jnp.where(bucket // LANES == n, other, stiff)
            face = [jnp.broadcast_to(geo_ref[t, q : q + 1, :], (8, LANES)) for q in range(3, 9)]
            total = [jnp.zeros((8, LANES), jnp.float32)] * 3
            for s in range(0, segs, 8):
                row = s // 16 * 96 + s % 16
                found = [
                    found_ref[row + 16 * q : row + 16 * q + 8, k * LANES : (k + 1) * LANES] for q in range(6)
                ]
                d, m = found[:3], found[3:]
                dist = d[0] * d[0] + d[1] * d[1] + d[2] * d[2]
                depth = d[0] * m[0] + d[1] * m[1] + d[2] * m[2]
                area = face[0] * m[0] + face[1] * m[1] + face[2] * m[2]
                closing = face[3] * m[0] + face[4] * m[1] + face[5] * m[2]
                traction = (jnp.exp2(-dist) * jnp.maximum(depth, 0.0)) * (
                    (stiff - closing) * jnp.abs(area)
                )
                total = [total[c] + traction * m[c] for c in range(3)]
            for c in range(3):
                row = c * tiles + t
                force_ref[row : row + 1, :] = jnp.sum(total[c], axis=0, keepdims=True)

    pipelined(tiles // per_step, gather, force, found0_ref, found1_ref)


def last_kernel(mine_ref, other_ref, force_ref):
    tiles = mine_ref.shape[0] // 3
    for t in range(tiles):
        at = pl.ds(t, 3, stride=tiles)
        force_ref[:, t * LANES : (t + 1) * LANES] = mine_ref[at, :] + other_ref[at, :]


def swap(value, axis, mask):
    size = lax.axis_size(axis)
    return lax.ppermute(value, axis, [(i, i ^ mask) for i in range(size)])


def local(node_data, eroded, bucket_map, seg_point, seg_angle):
    elem_count = lax.axis_size("elem")
    bucket_split = lax.axis_size("bucket")
    held, _, segs = seg_point.shape
    buckets = held * elem_count
    erode_count = eroded.shape[0]
    faces = node_data.shape[1]
    tiles = SIDES * erode_count // LANES
    map_rows = faces // LANES
    wide = round_up(buckets, LANES)
    pay_rows = round_up(5 * held + wide // LANES, 8)
    step = 2 * LANES
    words = -(-(map_rows // 8) // (31 // max(1, (buckets - 1).bit_length())))
    inputs = (eroded.reshape(-1, LANES), bucket_map.reshape(-1, LANES), seg_point.transpose(1, 0, 2), seg_angle)

    pay, face_bucket, face_row, face_lane = pl.pallas_call(
        functools.partial(index_kernel, buckets),
        out_shape=(
            jax.ShapeDtypeStruct((pay_rows, LANES), jnp.float32),
            jax.ShapeDtypeStruct((tiles, LANES), jnp.int32),
            jax.ShapeDtypeStruct((tiles, LANES), jnp.int32),
            jax.ShapeDtypeStruct((tiles, LANES), jnp.int32),
        ),
        in_specs=[HBM] * 4,
        out_specs=[VMEM] * 4,
        scratch_shapes=[pltpu.VMEM(x.shape, x.dtype) for x in inputs]
        + [pltpu.VMEM((8 * words, LANES), jnp.int32), pltpu.SemaphoreType.DMA((4,))],
        name="index",
        compiler_params=pltpu.CompilerParams(vmem_limit_bytes=67043328),
        cost_estimate=pl.CostEstimate(flops=4_000_000, bytes_accessed=100_000, transcendentals=0),
    )(*inputs)

    nodes = node_data.reshape(3, 8, map_rows, LANES).transpose(0, 2, 1, 3).reshape(24 * map_rows, LANES)
    dense = pl.pallas_call(
        dense_kernel,
        out_shape=jax.ShapeDtypeStruct((9 * map_rows, 2 * LANES), jnp.bfloat16),
        in_specs=[VMEM],
        out_specs=VMEM,
        name="dense",
        compiler_params=pltpu.CompilerParams(vmem_limit_bytes=16 * 2**20),
        cost_estimate=pl.CostEstimate(flops=4_000_000, bytes_accessed=1_300_000, transcendentals=0),
    )(nodes)

    bits = elem_count.bit_length() - 1
    order = round_order(bits)
    tables = [pay]
    done = 0
    while done < bits:
        masks = [1 << order[done]]
        if done + 1 < bits:
            masks += [1 << order[done + 1], masks[0] + (1 << order[done + 1])]
        if done:
            tables, dense = lax.optimization_barrier((tables, dense))
            end = tables[0].shape[0] - pay_rows + 5 * held
            tables = [jnp.concatenate([x[:end] for x in tables] + [sum(x[end:] for x in tables)], axis=0)]
        tables += [swap(tables[0], "elem", m) for m in masks]
        done += 1 if len(masks) == 1 else 2

    geometry, corner = pl.pallas_call(
        face_kernel,
        out_shape=(
            jax.ShapeDtypeStruct((tiles, 16, LANES), jnp.float32),
            jax.ShapeDtypeStruct((tiles, 16, LANES), jnp.bfloat16),
        ),
        in_specs=[VMEM] * 3,
        out_specs=[VMEM] * 2,
        scratch_shapes=[
            pltpu.VMEM((9 * map_rows, step), jnp.float32),
            pltpu.VMEM((9 * map_rows, step), jnp.float32),
        ],
        name="faces",
        compiler_params=pltpu.CompilerParams(vmem_limit_bytes=16 * 2**20),
        cost_estimate=pl.CostEstimate(flops=8_000_000, bytes_accessed=500_000, transcendentals=0),
    )(dense, face_row, face_lane)

    columns = 3 * buckets + 16
    half = pl.pallas_call(
        functools.partial(table_kernel, held, segs),
        out_shape=jax.ShapeDtypeStruct((6 * segs, columns), jnp.bfloat16),
        in_specs=[VMEM],
        out_specs=VMEM,
        name="table",
        compiler_params=pltpu.CompilerParams(vmem_limit_bytes=16 * 2**20),
        cost_estimate=pl.CostEstimate(flops=4_000_000, bytes_accessed=100_000, transcendentals=0),
    )(tables[0])
    force = pl.pallas_call(
        lambda *refs: force_kernel(held, segs, order, refs[: len(tables)], refs[len(tables) :]),
        out_shape=jax.ShapeDtypeStruct((3 * tiles, LANES), jnp.float32),
        in_specs=[VMEM] * (4 + len(tables)),
        out_specs=VMEM,
        scratch_shapes=[
            pltpu.VMEM((6 * segs, columns), jnp.bfloat16),
            pltpu.VMEM((wide // LANES, LANES), jnp.float32),
            pltpu.VMEM((6 * segs, step), jnp.float32),
            pltpu.VMEM((6 * segs, step), jnp.float32),
        ],
        name="forces",
        compiler_params=pltpu.CompilerParams(vmem_limit_bytes=24 * 2**20),
        cost_estimate=pl.CostEstimate(flops=16_000_000, bytes_accessed=400_000, transcendentals=0),
    )(*tables, half, face_bucket, geometry, corner)

    bit = 1
    while 2 * bit < bucket_split:
        force = force + swap(force, "bucket", bit)
        bit *= 2
    return pl.pallas_call(
        last_kernel,
        out_shape=jax.ShapeDtypeStruct((3, tiles * LANES), jnp.float32),
        in_specs=[VMEM] * 2,
        out_specs=VMEM,
        name="last",
        compiler_params=pltpu.CompilerParams(vmem_limit_bytes=8 * 2**20),
    )(force, swap(force, "bucket", bit))


def solution(mesh):
    in_specs = (
        P(None, "elem"),
        P("elem"),
        P("elem"),
        P("elem", None, "bucket"),
        P("elem", None, "bucket"),
    )
    return jax.shard_map(local, mesh=mesh, in_specs=in_specs, out_specs=P(None, "elem"), check_vma=False)
```

```python
import functools
import math

import jax
import jax.numpy as jnp
from jax import lax
from jax.experimental import pallas as pl
from jax.experimental.pallas import tpu as pltpu
from jax.sharding import PartitionSpec as P

STIFFNESS = 20.0
DAMPING = 0.5
LANES = 128
SIDES = 6
KAPPA = math.sqrt(0.5 / math.log(2.0))


VMEM = pl.BlockSpec(memory_space=pltpu.VMEM)
HBM = pl.BlockSpec(memory_space=pltpu.HBM)


def lane_take(table, index):
    return jnp.take_along_axis(table, index, axis=1, mode="promise_in_bounds")


def round_order(bits):
    order = list(range(bits))
    return order[:1] + order[2:] + order[1:2]


def round_up(n, k):
    return (n + k - 1) // k * k


def fetch(pairs, sems):
    copies = [pltpu.make_async_copy(source, target, sems.at[k]) for k, (source, target) in enumerate(pairs)]
    for copy in copies:
        copy.start()
    return copies


def index_kernel(buckets, *refs):
    inputs, (pay_ref, bucket_ref, row_ref, lane_ref) = refs[:4], refs[4:8]
    eroded_ref, map_ref, point_ref, angle_ref, packed_ref, sems = refs[8:]
    copies = fetch(zip(inputs, (eroded_ref, map_ref, point_ref, angle_ref)), sems)
    groups = eroded_ref.shape[0]
    lane = lax.broadcasted_iota(jnp.int32, (groups, LANES), 1)
    ats = [part * LANES + lane for part in range(SIDES)]
    picks = [(at // SIDES, at % SIDES) for at in ats]
    bits = max(1, (buckets - 1).bit_length())
    words = packed_ref.shape[0] // 8
    copies[0].wait()
    eroded = SIDES * eroded_ref[...]
    for part in range(SIDES):
        at, side = picks[part]
        face = lane_take(eroded, at) + side
        row_ref[pl.ds(part, groups, stride=SIDES), :] = face >> 7
        lane_ref[pl.ds(part, groups, stride=SIDES), :] = face & (LANES - 1)
    tiles = groups * SIDES
    map_rows = map_ref.shape[0]
    sub = lax.broadcasted_iota(jnp.int32, (8, LANES), 0)
    bucket_iota = lax.broadcasted_iota(jnp.int32, (buckets, LANES), 0)
    copies[1].wait()
    for w in range(words):
        word = map_ref[8 * w : 8 * w + 8, :]
        for k in range(1, -(-(map_rows // 8 - w) // words)):
            r = 8 * (w + k * words)
            word = word | (map_ref[r : r + 8, :] << (bits * k))
        packed_ref[8 * w : 8 * w + 8, :] = word
    hist = jnp.zeros(bucket_iota.shape, jnp.float32)

    def tile(t, hist):
        at_lane = jnp.broadcast_to(lane_ref[pl.ds(t, 1), :], (8, LANES))
        row = jnp.broadcast_to(row_ref[pl.ds(t, 1), :], (8, LANES))
        group = row >> 3
        slot = sum(((group >= k * words).astype(jnp.int32) for k in range(1, -(-(map_rows // 8) // words))), 0)
        key = ((group - slot * words) << 3) + (row & 7) - sub
        found = jnp.zeros((8, LANES), jnp.int32)
        for w in range(words):
            found = jnp.where(key == 8 * w, lane_take(packed_ref[8 * w : 8 * w + 8, :], at_lane), found)
        found = jnp.sum(found, axis=0, keepdims=True)
        bucket = (found >> (bits * slot[0:1])) & (2**bits - 1)
        bucket_ref[pl.ds(t, 1), :] = bucket
        return hist + jnp.where(bucket_iota == bucket, 1.0, 0.0)

    unroll = tiles if buckets <= LANES else 2
    hist = lax.fori_loop(0, tiles, tile, hist, unroll=unroll)
    local = point_ref.shape[1]
    copies[2].wait()
    for c in range(3):
        pay_ref[c * local : (c + 1) * local, :] = point_ref[c]
    copies[3].wait()
    for c in range(2):
        pay_ref[(3 + c) * local : (4 + c) * local, :] = angle_ref[:, c, :]
    for k in range(0, buckets, LANES):
        block = hist[k : k + LANES, :]
        row = 5 * local + k // LANES
        pay_ref[row : row + 1, 0 : block.shape[0]] = jnp.sum(block.T, axis=0, keepdims=True)


def split(value, parts):
    pieces = []
    for _ in range(parts):
        piece = value.astype(jnp.bfloat16)
        pieces.append(piece)
        value = value - piece.astype(jnp.float32)
    return pieces


def dense_kernel(node_ref, dense_ref):
    map_rows = dense_ref.shape[0] // 9

    def dense(g, carry):
        values = [[] for _ in range(9)]
        for h in range(2):
            rows = []
            for k in range(24):
                start = (k // 8) * (map_rows * 8) + (2 * g + h) * 64 + k % 8
                rows.append(node_ref[pl.ds(start, 8, stride=8), :])
            corner = [rows[3 * k : 3 * k + 3] for k in range(4)]
            motion = [rows[12 + 3 * k : 15 + 3 * k] for k in range(4)]
            first = [corner[2][c] - corner[0][c] for c in range(3)]
            second = [corner[3][c] - corner[1][c] for c in range(3)]
            for c in range(3):
                u, v = (c + 1) % 3, (c + 2) % 3
                total = ((corner[0][c] + corner[1][c]) + corner[2][c]) + corner[3][c]
                values[c].append((0.25 * KAPPA) * total)
                values[3 + c].append((0.5 / KAPPA) * (first[u] * second[v] - first[v] * second[u]))
                total = ((motion[0][c] + motion[1][c]) + motion[2][c]) + motion[3][c]
                values[6 + c].append((0.25 * DAMPING) * total)
        for q in range(9):
            at = pl.ds(pl.multiple_of(q * map_rows + g * 16, 16), 16)
            high, low = split(jnp.concatenate(values[q], axis=0), 2)
            dense_ref[at, 0:LANES] = high
            dense_ref[at, LANES : 2 * LANES] = low
        return carry

    lax.fori_loop(0, map_rows // 16, dense, 0)


def face_kernel(dense_ref, row_ref, lane_ref, geo_ref, corner_ref, found0_ref, found1_ref):
    map_rows = dense_ref.shape[0] // 9
    step = found0_ref.shape[1]
    tiles = row_ref.shape[0]
    per_step = step // LANES
    lane_iota = lax.broadcasted_iota(jnp.int32, (LANES, LANES), 0)
    sub = lax.broadcasted_iota(jnp.int32, (8, LANES), 0)
    corner_ref[...] = jnp.zeros(corner_ref.shape, corner_ref.dtype)

    def gather(i, found_ref):
        hot = []
        for k in range(per_step):
            here = lane_iota == lane_ref[pl.ds(i * per_step + k, 1), :]
            hot.append(jnp.where(here, 1.0, 0.0).astype(jnp.bfloat16))
        hot = jnp.concatenate(hot, axis=1)
        hot = jnp.concatenate([hot, hot], axis=0)
        found_ref[...] = jnp.dot(dense_ref[...], hot, preferred_element_type=jnp.float32)

    def select(i, found_ref):
        for k in range(per_step):
            t = i * per_step + k
            at_row = jnp.broadcast_to(row_ref[pl.ds(t, 1), :], (8, LANES)) - sub
            found = [jnp.zeros((8, LANES), jnp.float32)] * 9
            for r in range(0, map_rows, 8):
                here = at_row == r
                for q in range(9):
                    at = q * map_rows + r
                    found[q] = jnp.where(here, found_ref[at : at + 8, k * LANES : (k + 1) * LANES], found[q])
            for q in range(9):
                geo_ref[t, q : q + 1, :] = jnp.sum(found[q], axis=0, keepdims=True)

    pipelined(tiles // per_step, gather, select, found0_ref, found1_ref)

    def pieces(t, carry):
        corner_ref[t, 0:9, :] = jnp.concatenate(split(geo_ref[t, 0:3, :], 3), axis=0)
        return carry

    lax.fori_loop(0, tiles, pieces, 0, unroll=4)


def pipelined(steps, produce, consume, ref0, ref1):
    refs = (ref0, ref1)
    produce(0, ref0)
    for i in range(steps):
        if i + 1 < steps:
            produce(i + 1, refs[(i + 1) % 2])
        consume(i, refs[i % 2])


def table_columns(refs, local):
    rows = [jnp.concatenate([r[c * local : (c + 1) * local, :] for r in refs], axis=0) for c in range(5)]
    azimuth, polar = rows[3], rows[4]
    ring = jnp.sin(polar)
    columns = [KAPPA * rows[0], KAPPA * rows[1], KAPPA * rows[2]]
    return columns + [jnp.cos(azimuth) * ring, jnp.sin(azimuth) * ring, jnp.cos(polar)]


def region(buckets):
    return round_up(3 * buckets + 9, LANES)


def put_table(table, local, segs, start, take_off, hot_ref):
    blocks = table.shape[0] // (5 * local)
    group = min(LANES // local, blocks)
    parts = [
        table_columns([table.at[5 * local * b :] for b in range(b0, b0 + group)], local)
        for b0 in range(0, blocks, group)
    ]
    rest = region(blocks * local) - 3 * blocks * local
    row = lax.broadcasted_iota(jnp.int32, (rest, segs), 0)
    for q in range(6):
        pieces = split(jnp.concatenate([part[q] for part in parts], axis=0), 3)
        pieces = [piece.astype(jnp.float32) for piece in pieces]
        tail = jnp.where((row % 3 == q) & (row < 9), -1.0, 0.0) if take_off else jnp.zeros(row.shape, jnp.float32)
        whole = jnp.concatenate(pieces + [tail], axis=0)
        for k in range(0, whole.shape[0], LANES):
            block = whole[k : k + LANES].T.astype(jnp.bfloat16)
            for g in range(0, segs, 16):
                at = 6 * g + 16 * q
                hot_ref[at : at + 16, start + k : start + k + LANES] = block[g : g + 16]


def table_kernel(local, segs, table_ref, hot_ref):
    put_table(table_ref, local, segs, 0, True, hot_ref)


def force_kernel(local, segs, order, tables, refs):
    half_ref, bucket_ref, geo_ref, corner_ref, force_ref, hot_ref, stiff_ref, found0_ref, found1_ref = refs
    per_table_buckets = tables[0].shape[0] // (5 * local) * local
    count_at = 5 * per_table_buckets
    tiles = bucket_ref.shape[0]
    wide = stiff_ref.shape[0] * LANES
    step = found0_ref.shape[1]
    per_step = step // LANES
    turn = lax.axis_index("elem") * local
    width = region(per_table_buckets)
    hot_ref[:, 0:width] = half_ref[...]
    for n, table in enumerate(tables[1:]):
        put_table(table, local, segs, (n + 1) * width, False, hot_ref)
    for k in range(wide // LANES):
        count = sum(table[count_at + k : count_at + k + 1, :] for table in tables)
        stiff_ref[k : k + 1, :] = STIFFNESS * lax.rsqrt(jnp.maximum(count, 1.0))
    sub = lax.broadcasted_iota(jnp.int32, (per_table_buckets, LANES), 0)

    def gather(i, found_ref):
        hot = []
        for k in range(per_step):
            t = i * per_step + k
            spot = bucket_ref[pl.ds(t, 1), :] ^ turn
            owner = sum(((spot // local >> bit) & 1) << k for k, bit in enumerate(order))
            spot = owner * local + spot % local
            rows = []
            for n in range(len(tables)):
                here = sub == spot - n * per_table_buckets
                rows += [jnp.where(here, 1.0, 0.0).astype(jnp.bfloat16)] * 3
                tail = width - 3 * per_table_buckets
                if n == 0:
                    rows.append(corner_ref[t])
                    tail -= 16
                rows.append(jnp.zeros((tail, LANES), jnp.bfloat16))
            hot.append(jnp.concatenate(rows, axis=0))
        hot = jnp.concatenate(hot, axis=1)
        found_ref[...] = jnp.dot(hot_ref[...], hot, preferred_element_type=jnp.float32)

    def force(i, found_ref):
        for k in range(per_step):
            t = i * per_step + k
            bucket = jnp.broadcast_to(bucket_ref[pl.ds(t, 1), :], (8, LANES))
            stiff = lane_take(jnp.broadcast_to(stiff_ref[0:1, :], (8, LANES)), bucket % LANES)
            for n in range(1, wide // LANES):
                other = lane_take(jnp.broadcast_to(stiff_ref[n : n + 1, :], (8, LANES)), bucket % LANES)
                stiff = jnp.where(bucket // LANES == n, other, stiff)
            face = [jnp.broadcast_to(geo_ref[t, q : q + 1, :], (8, LANES)) for q in range(3, 9)]
            total = [jnp.zeros((8, LANES), jnp.float32)] * 3
            for s in range(0, segs, 8):
                row = s // 16 * 96 + s % 16
                found = [
                    found_ref[row + 16 * q : row + 16 * q + 8, k * LANES : (k + 1) * LANES] for q in range(6)
                ]
                d, m = found[:3], found[3:]
                dist = d[0] * d[0] + d[1] * d[1] + d[2] * d[2]
                depth = d[0] * m[0] + d[1] * m[1] + d[2] * m[2]
                area = face[0] * m[0] + face[1] * m[1] + face[2] * m[2]
                closing = face[3] * m[0] + face[4] * m[1] + face[5] * m[2]
                traction = (jnp.exp2(-dist) * jnp.maximum(depth, 0.0)) * (
                    (stiff - closing) * jnp.abs(area)
                )
                total = [total[c] + traction * m[c] for c in range(3)]
            for c in range(3):
                row = c * tiles + t
                force_ref[row : row + 1, :] = jnp.sum(total[c], axis=0, keepdims=True)

    pipelined(tiles // per_step, gather, force, found0_ref, found1_ref)


def last_kernel(mine_ref, other_ref, force_ref):
    tiles = mine_ref.shape[0] // 3
    for t in range(tiles):
        at = pl.ds(t, 3, stride=tiles)
        force_ref[:, t * LANES : (t + 1) * LANES] = mine_ref[at, :] + other_ref[at, :]


def swap(value, elem_mask, bucket_mask):
    elems, splits = lax.axis_size("elem"), lax.axis_size("bucket")
    pairs = [
        (e * splits + b, (e ^ elem_mask) * splits + (b ^ bucket_mask)) for e in range(elems) for b in range(splits)
    ]
    return lax.ppermute(value, ("elem", "bucket"), pairs)


def local(node_data, eroded, bucket_map, seg_point, seg_angle):
    elem_count = lax.axis_size("elem")
    bucket_split = lax.axis_size("bucket")
    held, _, segs = seg_point.shape
    buckets = held * elem_count
    erode_count = eroded.shape[0]
    faces = node_data.shape[1]
    tiles = SIDES * erode_count // LANES
    map_rows = faces // LANES
    wide = round_up(buckets, LANES)
    pay_rows = round_up(5 * held + wide // LANES, 8)
    step = 2 * LANES
    words = -(-(map_rows // 8) // (31 // max(1, (buckets - 1).bit_length())))
    inputs = (eroded.reshape(-1, LANES), bucket_map.reshape(-1, LANES), seg_point.transpose(1, 0, 2), seg_angle)

    pay, face_bucket, face_row, face_lane = pl.pallas_call(
        functools.partial(index_kernel, buckets),
        out_shape=(
            jax.ShapeDtypeStruct((pay_rows, LANES), jnp.float32),
            jax.ShapeDtypeStruct((tiles, LANES), jnp.int32),
            jax.ShapeDtypeStruct((tiles, LANES), jnp.int32),
            jax.ShapeDtypeStruct((tiles, LANES), jnp.int32),
        ),
        in_specs=[HBM] * 4,
        out_specs=[VMEM] * 4,
        scratch_shapes=[pltpu.VMEM(x.shape, x.dtype) for x in inputs]
        + [pltpu.VMEM((8 * words, LANES), jnp.int32), pltpu.SemaphoreType.DMA((4,))],
        name="index",
        compiler_params=pltpu.CompilerParams(vmem_limit_bytes=67043328),
        cost_estimate=pl.CostEstimate(flops=4_000_000, bytes_accessed=100_000, transcendentals=0),
    )(*inputs)

    nodes = node_data.reshape(3, 8, map_rows, LANES).transpose(0, 2, 1, 3).reshape(24 * map_rows, LANES)
    dense = pl.pallas_call(
        dense_kernel,
        out_shape=jax.ShapeDtypeStruct((9 * map_rows, 2 * LANES), jnp.bfloat16),
        in_specs=[VMEM],
        out_specs=VMEM,
        name="dense",
        compiler_params=pltpu.CompilerParams(vmem_limit_bytes=16 * 2**20),
        cost_estimate=pl.CostEstimate(flops=4_000_000, bytes_accessed=1_300_000, transcendentals=0),
    )(nodes)

    bits = elem_count.bit_length() - 1
    order = round_order(bits)
    tables = [pay]
    done = 0
    while done < bits:
        masks = [1 << order[done]]
        if done + 1 < bits:
            masks += [1 << order[done + 1], masks[0] + (1 << order[done + 1])]
        if done:
            tables, dense = lax.optimization_barrier((tables, dense))
            end = tables[0].shape[0] - pay_rows + 5 * held
            tables = [jnp.concatenate([x[:end] for x in tables] + [sum(x[end:] for x in tables)], axis=0)]
        tables += [swap(tables[0], m, 1) for m in masks]
        done += 1 if len(masks) == 1 else 2

    geometry, corner = pl.pallas_call(
        face_kernel,
        out_shape=(
            jax.ShapeDtypeStruct((tiles, 16, LANES), jnp.float32),
            jax.ShapeDtypeStruct((tiles, 16, LANES), jnp.bfloat16),
        ),
        in_specs=[VMEM] * 3,
        out_specs=[VMEM] * 2,
        scratch_shapes=[
            pltpu.VMEM((9 * map_rows, step), jnp.float32),
            pltpu.VMEM((9 * map_rows, step), jnp.float32),
        ],
        name="faces",
        compiler_params=pltpu.CompilerParams(vmem_limit_bytes=16 * 2**20),
        cost_estimate=pl.CostEstimate(flops=8_000_000, bytes_accessed=500_000, transcendentals=0),
    )(dense, face_row, face_lane)

    width = region(tables[0].shape[0] // (5 * held) * held)
    half = pl.pallas_call(
        functools.partial(table_kernel, held, segs),
        out_shape=jax.ShapeDtypeStruct((6 * segs, width), jnp.bfloat16),
        in_specs=[VMEM],
        out_specs=VMEM,
        name="table",
        compiler_params=pltpu.CompilerParams(vmem_limit_bytes=16 * 2**20),
        cost_estimate=pl.CostEstimate(flops=4_000_000, bytes_accessed=100_000, transcendentals=0),
    )(tables[0])
    force = pl.pallas_call(
        lambda *refs: force_kernel(held, segs, order, refs[: len(tables)], refs[len(tables) :]),
        out_shape=jax.ShapeDtypeStruct((3 * tiles, LANES), jnp.float32),
        in_specs=[VMEM] * (4 + len(tables)),
        out_specs=VMEM,
        scratch_shapes=[
            pltpu.VMEM((6 * segs, len(tables) * width), jnp.bfloat16),
            pltpu.VMEM((wide // LANES, LANES), jnp.float32),
            pltpu.VMEM((6 * segs, step), jnp.float32),
            pltpu.VMEM((6 * segs, step), jnp.float32),
        ],
        name="forces",
        compiler_params=pltpu.CompilerParams(vmem_limit_bytes=24 * 2**20),
        cost_estimate=pl.CostEstimate(flops=16_000_000, bytes_accessed=400_000, transcendentals=0),
    )(*tables, half, face_bucket, geometry, corner)

    force = force + swap(force, 0, 1)
    mask = 3
    while mask + 1 < bucket_split:
        force = force + swap(force, 0, mask)
        mask = 2 * mask + 1
    return pl.pallas_call(
        last_kernel,
        out_shape=jax.ShapeDtypeStruct((3, tiles * LANES), jnp.float32),
        in_specs=[VMEM] * 2,
        out_specs=VMEM,
        name="last",
        compiler_params=pltpu.CompilerParams(vmem_limit_bytes=8 * 2**20),
    )(force, swap(force, 0, mask))


def solution(mesh):
    in_specs = (
        P(None, "elem"),
        P("elem"),
        P("elem"),
        P("elem", None, "bucket"),
        P("elem", None, "bucket"),
    )
    return jax.shard_map(local, mesh=mesh, in_specs=in_specs, out_specs=P(None, "elem"), check_vma=False)
```

```python
import functools
import math

import jax
import jax.numpy as jnp
from jax import lax
from jax.experimental import pallas as pl
from jax.experimental.pallas import tpu as pltpu
from jax.sharding import PartitionSpec as P

STIFFNESS = 20.0
DAMPING = 0.5
LANES = 128
SIDES = 6
KAPPA = math.sqrt(0.5 / math.log(2.0))


VMEM = pl.BlockSpec(memory_space=pltpu.VMEM)
HBM = pl.BlockSpec(memory_space=pltpu.HBM)


def lane_take(table, index):
    return jnp.take_along_axis(table, index, axis=1, mode="promise_in_bounds")


def round_order(bits):
    order = list(range(bits))
    return order[:1] + order[2:] + order[1:2]


def round_up(n, k):
    return (n + k - 1) // k * k


def fetch(pairs, sems):
    copies = [pltpu.make_async_copy(source, target, sems.at[k]) for k, (source, target) in enumerate(pairs)]
    for copy in copies:
        copy.start()
    return copies


def index_kernel(buckets, *refs):
    inputs, (pay_ref, bucket_ref, row_ref, lane_ref) = refs[:4], refs[4:8]
    eroded_ref, map_ref, point_ref, angle_ref, packed_ref, sems = refs[8:]
    copies = fetch(zip(inputs, (eroded_ref, map_ref, point_ref, angle_ref)), sems)
    groups = eroded_ref.shape[0]
    lane = lax.broadcasted_iota(jnp.int32, (groups, LANES), 1)
    ats = [part * LANES + lane for part in range(SIDES)]
    picks = [(at // SIDES, at % SIDES) for at in ats]
    bits = max(1, (buckets - 1).bit_length())
    words = packed_ref.shape[0] // 8
    copies[0].wait()
    eroded = SIDES * eroded_ref[...]
    for part in range(SIDES):
        at, side = picks[part]
        face = lane_take(eroded, at) + side
        row_ref[pl.ds(part, groups, stride=SIDES), :] = face >> 7
        lane_ref[pl.ds(part, groups, stride=SIDES), :] = face & (LANES - 1)
    tiles = groups * SIDES
    map_rows = map_ref.shape[0]
    sub = lax.broadcasted_iota(jnp.int32, (8, LANES), 0)
    bucket_iota = lax.broadcasted_iota(jnp.int32, (buckets, LANES), 0)
    copies[1].wait()
    for w in range(words):
        word = map_ref[8 * w : 8 * w + 8, :]
        for k in range(1, -(-(map_rows // 8 - w) // words)):
            r = 8 * (w + k * words)
            word = word | (map_ref[r : r + 8, :] << (bits * k))
        packed_ref[8 * w : 8 * w + 8, :] = word
    hist = jnp.zeros(bucket_iota.shape, jnp.float32)

    def tile(t, hist):
        at_lane = jnp.broadcast_to(lane_ref[pl.ds(t, 1), :], (8, LANES))
        row = jnp.broadcast_to(row_ref[pl.ds(t, 1), :], (8, LANES))
        group = row >> 3
        slot = sum(((group >= k * words).astype(jnp.int32) for k in range(1, -(-(map_rows // 8) // words))), 0)
        key = ((group - slot * words) << 3) + (row & 7) - sub
        found = jnp.zeros((8, LANES), jnp.int32)
        for w in range(words):
            found = jnp.where(key == 8 * w, lane_take(packed_ref[8 * w : 8 * w + 8, :], at_lane), found)
        found = jnp.sum(found, axis=0, keepdims=True)
        bucket = (found >> (bits * slot[0:1])) & (2**bits - 1)
        bucket_ref[pl.ds(t, 1), :] = bucket
        return hist + jnp.where(bucket_iota == bucket, 1.0, 0.0)

    unroll = tiles if buckets <= LANES else 2
    hist = lax.fori_loop(0, tiles, tile, hist, unroll=unroll)
    local = point_ref.shape[1]
    copies[2].wait()
    for c in range(3):
        pay_ref[c * local : (c + 1) * local, :] = point_ref[c]
    copies[3].wait()
    for c in range(2):
        pay_ref[(3 + c) * local : (4 + c) * local, :] = angle_ref[:, c, :]
    for k in range(0, buckets, LANES):
        block = hist[k : k + LANES, :]
        row = 5 * local + k // LANES
        pay_ref[row : row + 1, 0 : block.shape[0]] = jnp.sum(block.T, axis=0, keepdims=True)


def split(value, parts):
    pieces = []
    for _ in range(parts):
        piece = value.astype(jnp.bfloat16)
        pieces.append(piece)
        value = value - piece.astype(jnp.float32)
    return pieces


def dense_kernel(node_ref, dense_ref):
    map_rows = dense_ref.shape[0] // 9

    def dense(g, carry):
        values = [[] for _ in range(9)]
        for h in range(2):
            rows = []
            for k in range(24):
                start = (k // 8) * (map_rows * 8) + (2 * g + h) * 64 + k % 8
                rows.append(node_ref[pl.ds(start, 8, stride=8), :])
            corner = [rows[3 * k : 3 * k + 3] for k in range(4)]
            motion = [rows[12 + 3 * k : 15 + 3 * k] for k in range(4)]
            first = [corner[2][c] - corner[0][c] for c in range(3)]
            second = [corner[3][c] - corner[1][c] for c in range(3)]
            for c in range(3):
                u, v = (c + 1) % 3, (c + 2) % 3
                total = ((corner[0][c] + corner[1][c]) + corner[2][c]) + corner[3][c]
                values[c].append((0.25 * KAPPA) * total)
                values[3 + c].append((0.5 / KAPPA) * (first[u] * second[v] - first[v] * second[u]))
                total = ((motion[0][c] + motion[1][c]) + motion[2][c]) + motion[3][c]
                values[6 + c].append((0.25 * DAMPING) * total)
        for q in range(9):
            at = pl.ds(pl.multiple_of(q * map_rows + g * 16, 16), 16)
            high, low = split(jnp.concatenate(values[q], axis=0), 2)
            dense_ref[at, 0:LANES] = high
            dense_ref[at, LANES : 2 * LANES] = low
        return carry

    lax.fori_loop(0, map_rows // 16, dense, 0)


def face_kernel(dense_ref, row_ref, lane_ref, geo_ref, corner_ref, found0_ref, found1_ref):
    map_rows = dense_ref.shape[0] // 9
    step = found0_ref.shape[1]
    tiles = row_ref.shape[0]
    per_step = step // LANES
    lane_iota = lax.broadcasted_iota(jnp.int32, (LANES, LANES), 0)
    sub = lax.broadcasted_iota(jnp.int32, (8, LANES), 0)
    corner_ref[...] = jnp.zeros(corner_ref.shape, corner_ref.dtype)

    def gather(i, found_ref):
        hot = []
        for k in range(per_step):
            here = lane_iota == lane_ref[pl.ds(i * per_step + k, 1), :]
            hot.append(jnp.where(here, 1.0, 0.0).astype(jnp.bfloat16))
        hot = jnp.concatenate(hot, axis=1)
        hot = jnp.concatenate([hot, hot], axis=0)
        found_ref[...] = jnp.dot(dense_ref[...], hot, preferred_element_type=jnp.float32)

    def select(i, found_ref):
        for k in range(per_step):
            t = i * per_step + k
            at_row = jnp.broadcast_to(row_ref[pl.ds(t, 1), :], (8, LANES)) - sub
            found = [jnp.zeros((8, LANES), jnp.float32)] * 9
            for r in range(0, map_rows, 8):
                here = at_row == r
                for q in range(9):
                    at = q * map_rows + r
                    found[q] = jnp.where(here, found_ref[at : at + 8, k * LANES : (k + 1) * LANES], found[q])
            for q in range(9):
                geo_ref[t, q : q + 1, :] = jnp.sum(found[q], axis=0, keepdims=True)

    pipelined(tiles // per_step, gather, select, found0_ref, found1_ref)

    def pieces(t, carry):
        corner_ref[t, 0:9, :] = jnp.concatenate(split(geo_ref[t, 0:3, :], 3), axis=0)
        return carry

    lax.fori_loop(0, tiles, pieces, 0, unroll=4)


def pipelined(steps, produce, consume, ref0, ref1):
    refs = (ref0, ref1)
    produce(0, ref0)
    for i in range(steps):
        if i + 1 < steps:
            produce(i + 1, refs[(i + 1) % 2])
        consume(i, refs[i % 2])


def table_columns(refs, local):
    rows = [jnp.concatenate([r[c * local : (c + 1) * local, :] for r in refs], axis=0) for c in range(5)]
    azimuth, polar = rows[3], rows[4]
    ring = jnp.sin(polar)
    columns = [KAPPA * rows[0], KAPPA * rows[1], KAPPA * rows[2]]
    return columns + [jnp.cos(azimuth) * ring, jnp.sin(azimuth) * ring, jnp.cos(polar)]


def region(buckets):
    return round_up(3 * buckets + 9, LANES)


def put_table(table, local, segs, start, take_off, hot_ref):
    blocks = table.shape[0] // (5 * local)
    group = min(LANES // local, blocks)
    parts = [
        table_columns([table.at[5 * local * b :] for b in range(b0, b0 + group)], local)
        for b0 in range(0, blocks, group)
    ]
    rest = region(blocks * local) - 3 * blocks * local
    row = lax.broadcasted_iota(jnp.int32, (rest, segs), 0)
    for q in range(6):
        pieces = split(jnp.concatenate([part[q] for part in parts], axis=0), 3)
        pieces = [piece.astype(jnp.float32) for piece in pieces]
        tail = jnp.where((row % 3 == q) & (row < 9), -1.0, 0.0) if take_off else jnp.zeros(row.shape, jnp.float32)
        whole = jnp.concatenate(pieces + [tail], axis=0)
        for k in range(0, whole.shape[0], LANES):
            block = whole[k : k + LANES].T.astype(jnp.bfloat16)
            for g in range(0, segs, 16):
                at = 6 * g + 16 * q
                hot_ref[at : at + 16, start + k : start + k + LANES] = block[g : g + 16]


def table_kernel(local, segs, table_ref, hot_ref):
    put_table(table_ref, local, segs, 0, True, hot_ref)


def spread_step(i, per_step, tables, per_table_buckets, local, order, bucket_ref, corner_ref):
    width = region(per_table_buckets)
    sub = lax.broadcasted_iota(jnp.int32, (per_table_buckets, LANES), 0)
    hot = []
    for k in range(per_step):
        t = i * per_step + k
        spot = bucket_ref[t : t + 1, :] ^ (lax.axis_index("elem") * local)
        owner = sum(((spot // local >> bit) & 1) << k for k, bit in enumerate(order))
        spot = owner * local + spot % local
        rows = []
        for n in range(tables):
            here = sub == spot - n * per_table_buckets
            rows += [jnp.where(here, 1.0, 0.0).astype(jnp.bfloat16)] * 3
            tail = width - 3 * per_table_buckets
            if n == 0:
                rows.append(corner_ref[t])
                tail -= 16
            rows.append(jnp.zeros((tail, LANES), jnp.bfloat16))
        hot.append(jnp.concatenate(rows, axis=0))
    return jnp.concatenate(hot, axis=1)


def spread_kernel(tables, per_table_buckets, local, order, bucket_ref, corner_ref, spread_ref):
    steps, _, step = spread_ref.shape
    for i in range(steps):
        spread_ref[i] = spread_step(
            i, step // LANES, tables, per_table_buckets, local, order, bucket_ref, corner_ref
        )


def force_kernel(local, segs, order, ahead, tables, refs):
    half_ref, bucket_ref, geo_ref, spread_ref, force_ref, hot_ref, stiff_ref, found0_ref, found1_ref = refs
    spread_refs = (bucket_ref, spread_ref)
    per_table_buckets = tables[0].shape[0] // (5 * local) * local
    count_at = 5 * per_table_buckets
    tiles = bucket_ref.shape[0]
    wide = stiff_ref.shape[0] * LANES
    step = found0_ref.shape[1]
    per_step = step // LANES
    width = region(per_table_buckets)
    hot_ref[:, 0:width] = half_ref[...]
    for n, table in enumerate(tables[1:]):
        put_table(table, local, segs, (n + 1) * width, False, hot_ref)
    for k in range(wide // LANES):
        count = sum(table[count_at + k : count_at + k + 1, :] for table in tables)
        stiff_ref[k : k + 1, :] = STIFFNESS * lax.rsqrt(jnp.maximum(count, 1.0))

    def gather(i, found_ref):
        if ahead:
            spread = spread_ref[i]
        else:
            spread = spread_step(i, per_step, len(tables), per_table_buckets, local, order, *spread_refs)
        found_ref[...] = jnp.dot(hot_ref[...], spread, preferred_element_type=jnp.float32)

    def force(i, found_ref):
        for k in range(per_step):
            t = i * per_step + k
            bucket = jnp.broadcast_to(bucket_ref[pl.ds(t, 1), :], (8, LANES))
            stiff = lane_take(jnp.broadcast_to(stiff_ref[0:1, :], (8, LANES)), bucket % LANES)
            for n in range(1, wide // LANES):
                other = lane_take(jnp.broadcast_to(stiff_ref[n : n + 1, :], (8, LANES)), bucket % LANES)
                stiff = jnp.where(bucket // LANES == n, other, stiff)
            face = [jnp.broadcast_to(geo_ref[t, q : q + 1, :], (8, LANES)) for q in range(3, 9)]
            total = [jnp.zeros((8, LANES), jnp.float32)] * 3
            for s in range(0, segs, 8):
                row = s // 16 * 96 + s % 16
                found = [
                    found_ref[row + 16 * q : row + 16 * q + 8, k * LANES : (k + 1) * LANES] for q in range(6)
                ]
                d, m = found[:3], found[3:]
                dist = d[0] * d[0] + d[1] * d[1] + d[2] * d[2]
                depth = d[0] * m[0] + d[1] * m[1] + d[2] * m[2]
                area = face[0] * m[0] + face[1] * m[1] + face[2] * m[2]
                closing = face[3] * m[0] + face[4] * m[1] + face[5] * m[2]
                traction = (jnp.exp2(-dist) * jnp.maximum(depth, 0.0)) * (
                    (stiff - closing) * jnp.abs(area)
                )
                total = [total[c] + traction * m[c] for c in range(3)]
            for c in range(3):
                row = c * tiles + t
                force_ref[row : row + 1, :] = jnp.sum(total[c], axis=0, keepdims=True)

    pipelined(tiles // per_step, gather, force, found0_ref, found1_ref)


def last_kernel(mine_ref, other_ref, force_ref):
    tiles = mine_ref.shape[0] // 3
    for t in range(tiles):
        at = pl.ds(t, 3, stride=tiles)
        force_ref[:, t * LANES : (t + 1) * LANES] = mine_ref[at, :] + other_ref[at, :]


def swap(value, elem_mask, bucket_mask):
    elems, splits = lax.axis_size("elem"), lax.axis_size("bucket")
    pairs = [
        (e * splits + b, (e ^ elem_mask) * splits + (b ^ bucket_mask)) for e in range(elems) for b in range(splits)
    ]
    return lax.ppermute(value, ("elem", "bucket"), pairs)


def local(node_data, eroded, bucket_map, seg_point, seg_angle):
    elem_count = lax.axis_size("elem")
    bucket_split = lax.axis_size("bucket")
    held, _, segs = seg_point.shape
    buckets = held * elem_count
    erode_count = eroded.shape[0]
    faces = node_data.shape[1]
    tiles = SIDES * erode_count // LANES
    map_rows = faces // LANES
    wide = round_up(buckets, LANES)
    pay_rows = round_up(5 * held + wide // LANES, 8)
    step = 2 * LANES
    words = -(-(map_rows // 8) // (31 // max(1, (buckets - 1).bit_length())))
    inputs = (eroded.reshape(-1, LANES), bucket_map.reshape(-1, LANES), seg_point.transpose(1, 0, 2), seg_angle)

    pay, face_bucket, face_row, face_lane = pl.pallas_call(
        functools.partial(index_kernel, buckets),
        out_shape=(
            jax.ShapeDtypeStruct((pay_rows, LANES), jnp.float32),
            jax.ShapeDtypeStruct((tiles, LANES), jnp.int32),
            jax.ShapeDtypeStruct((tiles, LANES), jnp.int32),
            jax.ShapeDtypeStruct((tiles, LANES), jnp.int32),
        ),
        in_specs=[HBM] * 4,
        out_specs=[VMEM] * 4,
        scratch_shapes=[pltpu.VMEM(x.shape, x.dtype) for x in inputs]
        + [pltpu.VMEM((8 * words, LANES), jnp.int32), pltpu.SemaphoreType.DMA((4,))],
        name="index",
        compiler_params=pltpu.CompilerParams(vmem_limit_bytes=67043328),
        cost_estimate=pl.CostEstimate(flops=4_000_000, bytes_accessed=100_000, transcendentals=0),
    )(*inputs)

    nodes = node_data.reshape(3, 8, map_rows, LANES).transpose(0, 2, 1, 3).reshape(24 * map_rows, LANES)
    dense = pl.pallas_call(
        dense_kernel,
        out_shape=jax.ShapeDtypeStruct((9 * map_rows, 2 * LANES), jnp.bfloat16),
        in_specs=[VMEM],
        out_specs=VMEM,
        name="dense",
        compiler_params=pltpu.CompilerParams(vmem_limit_bytes=16 * 2**20),
        cost_estimate=pl.CostEstimate(flops=4_000_000, bytes_accessed=1_300_000, transcendentals=0),
    )(nodes)

    bits = elem_count.bit_length() - 1
    order = round_order(bits)
    tables = [pay]
    done = 0
    while done < bits:
        masks = [1 << order[done]]
        if done + 1 < bits:
            masks += [1 << order[done + 1], masks[0] + (1 << order[done + 1])]
        if done:
            tables, dense = lax.optimization_barrier((tables, dense))
            end = tables[0].shape[0] - pay_rows + 5 * held
            tables = [jnp.concatenate([x[:end] for x in tables] + [sum(x[end:] for x in tables)], axis=0)]
        tables += [swap(tables[0], m, 1) for m in masks]
        done += 1 if len(masks) == 1 else 2

    geometry, corner = pl.pallas_call(
        face_kernel,
        out_shape=(
            jax.ShapeDtypeStruct((tiles, 16, LANES), jnp.float32),
            jax.ShapeDtypeStruct((tiles, 16, LANES), jnp.bfloat16),
        ),
        in_specs=[VMEM] * 3,
        out_specs=[VMEM] * 2,
        scratch_shapes=[
            pltpu.VMEM((9 * map_rows, step), jnp.float32),
            pltpu.VMEM((9 * map_rows, step), jnp.float32),
        ],
        name="faces",
        compiler_params=pltpu.CompilerParams(vmem_limit_bytes=16 * 2**20),
        cost_estimate=pl.CostEstimate(flops=8_000_000, bytes_accessed=500_000, transcendentals=0),
    )(dense, face_row, face_lane)

    width = region(tables[0].shape[0] // (5 * held) * held)
    half = pl.pallas_call(
        functools.partial(table_kernel, held, segs),
        out_shape=jax.ShapeDtypeStruct((6 * segs, width), jnp.bfloat16),
        in_specs=[VMEM],
        out_specs=VMEM,
        name="table",
        compiler_params=pltpu.CompilerParams(vmem_limit_bytes=16 * 2**20),
        cost_estimate=pl.CostEstimate(flops=4_000_000, bytes_accessed=100_000, transcendentals=0),
    )(tables[0])
    spread = corner
    ahead = len(tables) * width * tiles * LANES * 2 <= 4 * 2**20
    if ahead:
        per_table_buckets = tables[0].shape[0] // (5 * held) * held
        spread = pl.pallas_call(
            functools.partial(spread_kernel, len(tables), per_table_buckets, held, order),
            out_shape=jax.ShapeDtypeStruct((tiles * LANES // step, len(tables) * width, step), jnp.bfloat16),
            in_specs=[VMEM] * 2,
            out_specs=VMEM,
            name="spread",
            compiler_params=pltpu.CompilerParams(vmem_limit_bytes=16 * 2**20),
            cost_estimate=pl.CostEstimate(flops=2_000_000, bytes_accessed=100_000, transcendentals=0),
        )(face_bucket, corner)
    force = pl.pallas_call(
        lambda *refs: force_kernel(held, segs, order, ahead, refs[: len(tables)], refs[len(tables) :]),
        out_shape=jax.ShapeDtypeStruct((3 * tiles, LANES), jnp.float32),
        in_specs=[VMEM] * (4 + len(tables)),
        out_specs=VMEM,
        scratch_shapes=[
            pltpu.VMEM((6 * segs, len(tables) * width), jnp.bfloat16),
            pltpu.VMEM((wide // LANES, LANES), jnp.float32),
            pltpu.VMEM((6 * segs, step), jnp.float32),
            pltpu.VMEM((6 * segs, step), jnp.float32),
        ],
        name="forces",
        compiler_params=pltpu.CompilerParams(vmem_limit_bytes=24 * 2**20),
        cost_estimate=pl.CostEstimate(flops=16_000_000, bytes_accessed=400_000, transcendentals=0),
    )(*tables, half, face_bucket, geometry, spread)

    force = force + swap(force, 0, 1)
    mask = 3
    while mask + 1 < bucket_split:
        force = force + swap(force, 0, mask)
        mask = 2 * mask + 1
    return pl.pallas_call(
        last_kernel,
        out_shape=jax.ShapeDtypeStruct((3, tiles * LANES), jnp.float32),
        in_specs=[VMEM] * 2,
        out_specs=VMEM,
        name="last",
        compiler_params=pltpu.CompilerParams(vmem_limit_bytes=8 * 2**20),
    )(force, swap(force, 0, mask))


def solution(mesh):
    in_specs = (
        P(None, "elem"),
        P("elem"),
        P("elem"),
        P("elem", None, "bucket"),
        P("elem", None, "bucket"),
    )
    return jax.shard_map(local, mesh=mesh, in_specs=in_specs, out_specs=P(None, "elem"), check_vma=False)
```

```python
import functools
import math

import jax
import jax.numpy as jnp
from jax import lax
from jax.experimental import pallas as pl
from jax.experimental.pallas import tpu as pltpu
from jax.sharding import PartitionSpec as P

STIFFNESS = 20.0
DAMPING = 0.5
LANES = 128
SIDES = 6
KAPPA = math.sqrt(0.5 / math.log(2.0))


VMEM = pl.BlockSpec(memory_space=pltpu.VMEM)
HBM = pl.BlockSpec(memory_space=pltpu.HBM)


def lane_take(table, index):
    return jnp.take_along_axis(table, index, axis=1, mode="promise_in_bounds")


def round_order(bits):
    order = list(range(bits))
    return order[:1] + order[2:] + order[1:2]


def round_up(n, k):
    return (n + k - 1) // k * k


def fetch(pairs, sems):
    copies = [pltpu.make_async_copy(source, target, sems.at[k]) for k, (source, target) in enumerate(pairs)]
    for copy in copies:
        copy.start()
    return copies


def index_kernel(buckets, *refs):
    inputs, outputs = refs[:4], refs[4:8]
    eroded_ref, map_ref, point_ref, angle_ref, packed_ref, sems = refs[8:14]
    pay_ref, bucket_ref, row_ref, lane_ref, out_sems = refs[14:]
    copies = fetch(zip(inputs, (eroded_ref, map_ref, point_ref, angle_ref)), sems)
    groups = eroded_ref.shape[0]
    lane = lax.broadcasted_iota(jnp.int32, (groups, LANES), 1)
    ats = [part * LANES + lane for part in range(SIDES)]
    picks = [(at // SIDES, at % SIDES) for at in ats]
    bits = max(1, (buckets - 1).bit_length())
    words = packed_ref.shape[0] // 8
    copies[0].wait()
    eroded = SIDES * eroded_ref[...]
    for part in range(SIDES):
        at, side = picks[part]
        face = lane_take(eroded, at) + side
        row_ref[pl.ds(part, groups, stride=SIDES), :] = face >> 7
        lane_ref[pl.ds(part, groups, stride=SIDES), :] = face & (LANES - 1)
    tiles = groups * SIDES
    map_rows = map_ref.shape[0]
    sub = lax.broadcasted_iota(jnp.int32, (8, LANES), 0)
    bucket_iota = lax.broadcasted_iota(jnp.int32, (buckets, LANES), 0)
    copies[1].wait()
    for w in range(words):
        word = map_ref[8 * w : 8 * w + 8, :]
        for k in range(1, -(-(map_rows // 8 - w) // words)):
            r = 8 * (w + k * words)
            word = word | (map_ref[r : r + 8, :] << (bits * k))
        packed_ref[8 * w : 8 * w + 8, :] = word
    hist = jnp.zeros(bucket_iota.shape, jnp.float32)
    local = point_ref.shape[1]
    copies[2].wait()
    for c in range(3):
        pay_ref[c * local : (c + 1) * local, :] = point_ref[c]
    copies[3].wait()
    for c in range(2):
        pay_ref[(3 + c) * local : (4 + c) * local, :] = angle_ref[:, c, :]
    own, rest = pl.ds(0, 5 * local), pl.ds(5 * local, pay_ref.shape[0] - 5 * local)
    sent = [
        pltpu.make_async_copy(pay_ref.at[own, :], outputs[0].at[own, :], out_sems.at[0]),
        pltpu.make_async_copy(row_ref, outputs[2], out_sems.at[1]),
        pltpu.make_async_copy(lane_ref, outputs[3], out_sems.at[2]),
        pltpu.make_async_copy(bucket_ref, outputs[1], out_sems.at[3]),
        pltpu.make_async_copy(pay_ref.at[rest, :], outputs[0].at[rest, :], out_sems.at[4]),
    ]
    for copy in sent[:3]:
        copy.start()

    def tile(t, hist):
        at_lane = jnp.broadcast_to(lane_ref[pl.ds(t, 1), :], (8, LANES))
        row = jnp.broadcast_to(row_ref[pl.ds(t, 1), :], (8, LANES))
        group = row >> 3
        slot = sum(((group >= k * words).astype(jnp.int32) for k in range(1, -(-(map_rows // 8) // words))), 0)
        key = ((group - slot * words) << 3) + (row & 7) - sub
        found = jnp.zeros((8, LANES), jnp.int32)
        for w in range(words):
            found = jnp.where(key == 8 * w, lane_take(packed_ref[8 * w : 8 * w + 8, :], at_lane), found)
        found = jnp.sum(found, axis=0, keepdims=True)
        bucket = (found >> (bits * slot[0:1])) & (2**bits - 1)
        bucket_ref[pl.ds(t, 1), :] = bucket
        return hist + jnp.where(bucket_iota == bucket, 1.0, 0.0)

    unroll = tiles if buckets <= LANES else 2
    hist = lax.fori_loop(0, tiles, tile, hist, unroll=unroll)
    sent[3].start()
    for k in range(0, buckets, LANES):
        block = hist[k : k + LANES, :]
        row = 5 * local + k // LANES
        pay_ref[row : row + 1, 0 : block.shape[0]] = jnp.sum(block.T, axis=0, keepdims=True)
    sent[4].start()
    for copy in sent:
        copy.wait()


def split(value, parts):
    pieces = []
    for _ in range(parts):
        piece = value.astype(jnp.bfloat16)
        pieces.append(piece)
        value = value - piece.astype(jnp.float32)
    return pieces


def dense_kernel(node_ref, dense_ref):
    map_rows = dense_ref.shape[0] // 9

    def dense(g, carry):
        values = [[] for _ in range(9)]
        for h in range(2):
            rows = []
            for k in range(24):
                start = (k // 8) * (map_rows * 8) + (2 * g + h) * 64 + k % 8
                rows.append(node_ref[pl.ds(start, 8, stride=8), :])
            corner = [rows[3 * k : 3 * k + 3] for k in range(4)]
            motion = [rows[12 + 3 * k : 15 + 3 * k] for k in range(4)]
            first = [corner[2][c] - corner[0][c] for c in range(3)]
            second = [corner[3][c] - corner[1][c] for c in range(3)]
            for c in range(3):
                u, v = (c + 1) % 3, (c + 2) % 3
                total = ((corner[0][c] + corner[1][c]) + corner[2][c]) + corner[3][c]
                values[c].append((0.25 * KAPPA) * total)
                values[3 + c].append((0.5 / KAPPA) * (first[u] * second[v] - first[v] * second[u]))
                total = ((motion[0][c] + motion[1][c]) + motion[2][c]) + motion[3][c]
                values[6 + c].append((0.25 * DAMPING) * total)
        for q in range(9):
            at = pl.ds(pl.multiple_of(q * map_rows + g * 16, 16), 16)
            high, low = split(jnp.concatenate(values[q], axis=0), 2)
            dense_ref[at, 0:LANES] = high
            dense_ref[at, LANES : 2 * LANES] = low
        return carry

    lax.fori_loop(0, map_rows // 16, dense, 0)


def face_kernel(dense_ref, row_ref, lane_ref, geo_ref, corner_ref, found0_ref, found1_ref):
    map_rows = dense_ref.shape[0] // 9
    step = found0_ref.shape[1]
    tiles = row_ref.shape[0]
    per_step = step // LANES
    lane_iota = lax.broadcasted_iota(jnp.int32, (LANES, LANES), 0)
    sub = lax.broadcasted_iota(jnp.int32, (8, LANES), 0)
    corner_ref[...] = jnp.zeros(corner_ref.shape, corner_ref.dtype)

    def gather(i, found_ref):
        hot = []
        for k in range(per_step):
            here = lane_iota == lane_ref[pl.ds(i * per_step + k, 1), :]
            hot.append(jnp.where(here, 1.0, 0.0).astype(jnp.bfloat16))
        hot = jnp.concatenate(hot, axis=1)
        hot = jnp.concatenate([hot, hot], axis=0)
        found_ref[...] = jnp.dot(dense_ref[...], hot, preferred_element_type=jnp.float32)

    def select(i, found_ref):
        for k in range(per_step):
            t = i * per_step + k
            at_row = jnp.broadcast_to(row_ref[pl.ds(t, 1), :], (8, LANES)) - sub
            found = [jnp.zeros((8, LANES), jnp.float32)] * 9
            for r in range(0, map_rows, 8):
                here = at_row == r
                for q in range(9):
                    at = q * map_rows + r
                    found[q] = jnp.where(here, found_ref[at : at + 8, k * LANES : (k + 1) * LANES], found[q])
            for q in range(9):
                geo_ref[t, q : q + 1, :] = jnp.sum(found[q], axis=0, keepdims=True)

    pipelined(tiles // per_step, gather, select, found0_ref, found1_ref)

    def pieces(t, carry):
        corner_ref[t, 0:9, :] = jnp.concatenate(split(geo_ref[t, 0:3, :], 3), axis=0)
        return carry

    lax.fori_loop(0, tiles, pieces, 0, unroll=4)


def pipelined(steps, produce, consume, ref0, ref1):
    refs = (ref0, ref1)
    produce(0, ref0)
    for i in range(steps):
        if i + 1 < steps:
            produce(i + 1, refs[(i + 1) % 2])
        consume(i, refs[i % 2])


def table_columns(refs, local):
    rows = [jnp.concatenate([r[c * local : (c + 1) * local, :] for r in refs], axis=0) for c in range(5)]
    azimuth, polar = rows[3], rows[4]
    ring = jnp.sin(polar)
    columns = [KAPPA * rows[0], KAPPA * rows[1], KAPPA * rows[2]]
    return columns + [jnp.cos(azimuth) * ring, jnp.sin(azimuth) * ring, jnp.cos(polar)]


def region(buckets):
    return round_up(3 * buckets + 9, LANES)


def put_table(table, local, segs, start, take_off, hot_ref):
    blocks = table.shape[0] // (5 * local)
    group = min(LANES // local, blocks)
    parts = [
        table_columns([table.at[5 * local * b :] for b in range(b0, b0 + group)], local)
        for b0 in range(0, blocks, group)
    ]
    rest = region(blocks * local) - 3 * blocks * local
    row = lax.broadcasted_iota(jnp.int32, (rest, segs), 0)
    for q in range(6):
        pieces = split(jnp.concatenate([part[q] for part in parts], axis=0), 3)
        pieces = [piece.astype(jnp.float32) for piece in pieces]
        tail = jnp.where((row % 3 == q) & (row < 9), -1.0, 0.0) if take_off else jnp.zeros(row.shape, jnp.float32)
        whole = jnp.concatenate(pieces + [tail], axis=0)
        for k in range(0, whole.shape[0], LANES):
            block = whole[k : k + LANES].T.astype(jnp.bfloat16)
            for g in range(0, segs, 16):
                at = 6 * g + 16 * q
                hot_ref[at : at + 16, start + k : start + k + LANES] = block[g : g + 16]


def table_kernel(local, segs, table_ref, hot_ref):
    put_table(table_ref, local, segs, 0, True, hot_ref)


def spread_step(i, per_step, tables, per_table_buckets, local, order, bucket_ref, corner_ref):
    width = region(per_table_buckets)
    sub = lax.broadcasted_iota(jnp.int32, (per_table_buckets, LANES), 0)
    hot = []
    for k in range(per_step):
        t = i * per_step + k
        spot = bucket_ref[t : t + 1, :] ^ (lax.axis_index("elem") * local)
        owner = sum(((spot // local >> bit) & 1) << k for k, bit in enumerate(order))
        spot = owner * local + spot % local
        rows = []
        for n in range(tables):
            here = sub == spot - n * per_table_buckets
            rows += [jnp.where(here, 1.0, 0.0).astype(jnp.bfloat16)] * 3
            tail = width - 3 * per_table_buckets
            if n == 0:
                rows.append(corner_ref[t])
                tail -= 16
            rows.append(jnp.zeros((tail, LANES), jnp.bfloat16))
        hot.append(jnp.concatenate(rows, axis=0))
    return jnp.concatenate(hot, axis=1)


def spread_kernel(tables, per_table_buckets, local, order, bucket_ref, corner_ref, spread_ref):
    steps, _, step = spread_ref.shape
    for i in range(steps):
        spread_ref[i] = spread_step(
            i, step // LANES, tables, per_table_buckets, local, order, bucket_ref, corner_ref
        )


def force_kernel(local, segs, order, ahead, tables, refs):
    half_ref, bucket_ref, geo_ref, spread_ref, force_ref, hot_ref, stiff_ref, found0_ref, found1_ref = refs
    spread_refs = (bucket_ref, spread_ref)
    per_table_buckets = tables[0].shape[0] // (5 * local) * local
    count_at = 5 * per_table_buckets
    tiles = bucket_ref.shape[0]
    wide = stiff_ref.shape[0] * LANES
    step = found0_ref.shape[1]
    per_step = step // LANES
    width = region(per_table_buckets)
    hot_ref[:, 0:width] = half_ref[...]
    for n, table in enumerate(tables[1:]):
        put_table(table, local, segs, (n + 1) * width, False, hot_ref)
    for k in range(wide // LANES):
        count = sum(table[count_at + k : count_at + k + 1, :] for table in tables)
        stiff_ref[k : k + 1, :] = STIFFNESS * lax.rsqrt(jnp.maximum(count, 1.0))

    def gather(i, found_ref):
        if ahead:
            spread = spread_ref[i]
        else:
            spread = spread_step(i, per_step, len(tables), per_table_buckets, local, order, *spread_refs)
        found_ref[...] = jnp.dot(hot_ref[...], spread, preferred_element_type=jnp.float32)

    def force(i, found_ref):
        for k in range(per_step):
            t = i * per_step + k
            bucket = jnp.broadcast_to(bucket_ref[pl.ds(t, 1), :], (8, LANES))
            stiff = lane_take(jnp.broadcast_to(stiff_ref[0:1, :], (8, LANES)), bucket % LANES)
            for n in range(1, wide // LANES):
                other = lane_take(jnp.broadcast_to(stiff_ref[n : n + 1, :], (8, LANES)), bucket % LANES)
                stiff = jnp.where(bucket // LANES == n, other, stiff)
            face = [jnp.broadcast_to(geo_ref[t, q : q + 1, :], (8, LANES)) for q in range(3, 9)]
            total = [jnp.zeros((8, LANES), jnp.float32)] * 3
            for s in range(0, segs, 8):
                row = s // 16 * 96 + s % 16
                found = [
                    found_ref[row + 16 * q : row + 16 * q + 8, k * LANES : (k + 1) * LANES] for q in range(6)
                ]
                d, m = found[:3], found[3:]
                dist = d[0] * d[0] + d[1] * d[1] + d[2] * d[2]
                depth = d[0] * m[0] + d[1] * m[1] + d[2] * m[2]
                area = face[0] * m[0] + face[1] * m[1] + face[2] * m[2]
                closing = face[3] * m[0] + face[4] * m[1] + face[5] * m[2]
                traction = (jnp.exp2(-dist) * jnp.maximum(depth, 0.0)) * (
                    (stiff - closing) * jnp.abs(area)
                )
                total = [total[c] + traction * m[c] for c in range(3)]
            for c in range(3):
                row = c * tiles + t
                force_ref[row : row + 1, :] = jnp.sum(total[c], axis=0, keepdims=True)

    pipelined(tiles // per_step, gather, force, found0_ref, found1_ref)


def last_kernel(mine_ref, other_ref, force_ref):
    tiles = mine_ref.shape[0] // 3
    for t in range(tiles):
        at = pl.ds(t, 3, stride=tiles)
        force_ref[:, t * LANES : (t + 1) * LANES] = mine_ref[at, :] + other_ref[at, :]


def swap(value, elem_mask, bucket_mask):
    elems, splits = lax.axis_size("elem"), lax.axis_size("bucket")
    pairs = [
        (e * splits + b, (e ^ elem_mask) * splits + (b ^ bucket_mask)) for e in range(elems) for b in range(splits)
    ]
    return lax.ppermute(value, ("elem", "bucket"), pairs)


def local(node_data, eroded, bucket_map, seg_point, seg_angle):
    elem_count = lax.axis_size("elem")
    bucket_split = lax.axis_size("bucket")
    held, _, segs = seg_point.shape
    buckets = held * elem_count
    erode_count = eroded.shape[0]
    faces = node_data.shape[1]
    tiles = SIDES * erode_count // LANES
    map_rows = faces // LANES
    wide = round_up(buckets, LANES)
    pay_rows = round_up(5 * held + wide // LANES, 8)
    step = 2 * LANES
    words = -(-(map_rows // 8) // (31 // max(1, (buckets - 1).bit_length())))
    inputs = (eroded.reshape(-1, LANES), bucket_map.reshape(-1, LANES), seg_point.transpose(1, 0, 2), seg_angle)

    pay, face_bucket, face_row, face_lane = pl.pallas_call(
        functools.partial(index_kernel, buckets),
        out_shape=(
            jax.ShapeDtypeStruct((pay_rows, LANES), jnp.float32),
            jax.ShapeDtypeStruct((tiles, LANES), jnp.int32),
            jax.ShapeDtypeStruct((tiles, LANES), jnp.int32),
            jax.ShapeDtypeStruct((tiles, LANES), jnp.int32),
        ),
        in_specs=[HBM] * 4,
        out_specs=[HBM] * 4,
        scratch_shapes=[pltpu.VMEM(x.shape, x.dtype) for x in inputs]
        + [pltpu.VMEM((8 * words, LANES), jnp.int32), pltpu.SemaphoreType.DMA((4,))]
        + [pltpu.VMEM((pay_rows, LANES), jnp.float32)]
        + [pltpu.VMEM((tiles, LANES), jnp.int32)] * 3
        + [pltpu.SemaphoreType.DMA((5,))],
        name="index",
        compiler_params=pltpu.CompilerParams(vmem_limit_bytes=67043328),
        cost_estimate=pl.CostEstimate(flops=4_000_000, bytes_accessed=100_000, transcendentals=0),
    )(*inputs)

    nodes = node_data.reshape(3, 8, map_rows, LANES).transpose(0, 2, 1, 3).reshape(24 * map_rows, LANES)
    dense = pl.pallas_call(
        dense_kernel,
        out_shape=jax.ShapeDtypeStruct((9 * map_rows, 2 * LANES), jnp.bfloat16),
        in_specs=[VMEM],
        out_specs=VMEM,
        name="dense",
        compiler_params=pltpu.CompilerParams(vmem_limit_bytes=16 * 2**20),
        cost_estimate=pl.CostEstimate(flops=4_000_000, bytes_accessed=1_300_000, transcendentals=0),
    )(nodes)

    bits = elem_count.bit_length() - 1
    order = round_order(bits)
    tables = [pay]
    done = 0
    while done < bits:
        masks = [1 << order[done]]
        if done + 1 < bits:
            masks += [1 << order[done + 1], masks[0] + (1 << order[done + 1])]
        if done:
            tables, dense = lax.optimization_barrier((tables, dense))
            end = tables[0].shape[0] - pay_rows + 5 * held
            tables = [jnp.concatenate([x[:end] for x in tables] + [sum(x[end:] for x in tables)], axis=0)]
        tables += [swap(tables[0], m, 1) for m in masks]
        done += 1 if len(masks) == 1 else 2

    geometry, corner = pl.pallas_call(
        face_kernel,
        out_shape=(
            jax.ShapeDtypeStruct((tiles, 16, LANES), jnp.float32),
            jax.ShapeDtypeStruct((tiles, 16, LANES), jnp.bfloat16),
        ),
        in_specs=[VMEM] * 3,
        out_specs=[VMEM] * 2,
        scratch_shapes=[
            pltpu.VMEM((9 * map_rows, step), jnp.float32),
            pltpu.VMEM((9 * map_rows, step), jnp.float32),
        ],
        name="faces",
        compiler_params=pltpu.CompilerParams(vmem_limit_bytes=16 * 2**20),
        cost_estimate=pl.CostEstimate(flops=8_000_000, bytes_accessed=500_000, transcendentals=0),
    )(dense, face_row, face_lane)

    width = region(tables[0].shape[0] // (5 * held) * held)
    half = pl.pallas_call(
        functools.partial(table_kernel, held, segs),
        out_shape=jax.ShapeDtypeStruct((6 * segs, width), jnp.bfloat16),
        in_specs=[VMEM],
        out_specs=VMEM,
        name="table",
        compiler_params=pltpu.CompilerParams(vmem_limit_bytes=16 * 2**20),
        cost_estimate=pl.CostEstimate(flops=4_000_000, bytes_accessed=100_000, transcendentals=0),
    )(tables[0])
    spread = corner
    ahead = len(tables) * width * tiles * LANES * 2 <= 4 * 2**20
    if ahead:
        per_table_buckets = tables[0].shape[0] // (5 * held) * held
        spread = pl.pallas_call(
            functools.partial(spread_kernel, len(tables), per_table_buckets, held, order),
            out_shape=jax.ShapeDtypeStruct((tiles * LANES // step, len(tables) * width, step), jnp.bfloat16),
            in_specs=[VMEM] * 2,
            out_specs=VMEM,
            name="spread",
            compiler_params=pltpu.CompilerParams(vmem_limit_bytes=16 * 2**20),
            cost_estimate=pl.CostEstimate(flops=2_000_000, bytes_accessed=100_000, transcendentals=0),
        )(face_bucket, corner)
    force = pl.pallas_call(
        lambda *refs: force_kernel(held, segs, order, ahead, refs[: len(tables)], refs[len(tables) :]),
        out_shape=jax.ShapeDtypeStruct((3 * tiles, LANES), jnp.float32),
        in_specs=[VMEM] * (4 + len(tables)),
        out_specs=VMEM,
        scratch_shapes=[
            pltpu.VMEM((6 * segs, len(tables) * width), jnp.bfloat16),
            pltpu.VMEM((wide // LANES, LANES), jnp.float32),
            pltpu.VMEM((6 * segs, step), jnp.float32),
            pltpu.VMEM((6 * segs, step), jnp.float32),
        ],
        name="forces",
        compiler_params=pltpu.CompilerParams(vmem_limit_bytes=24 * 2**20),
        cost_estimate=pl.CostEstimate(flops=16_000_000, bytes_accessed=400_000, transcendentals=0),
    )(*tables, half, face_bucket, geometry, spread)

    force = force + swap(force, 0, 1)
    mask = 3
    while mask + 1 < bucket_split:
        force = force + swap(force, 0, mask)
        mask = 2 * mask + 1
    return pl.pallas_call(
        last_kernel,
        out_shape=jax.ShapeDtypeStruct((3, tiles * LANES), jnp.float32),
        in_specs=[VMEM] * 2,
        out_specs=VMEM,
        name="last",
        compiler_params=pltpu.CompilerParams(vmem_limit_bytes=8 * 2**20),
    )(force, swap(force, 0, mask))


def solution(mesh):
    in_specs = (
        P(None, "elem"),
        P("elem"),
        P("elem"),
        P("elem", None, "bucket"),
        P("elem", None, "bucket"),
    )
    return jax.shard_map(local, mesh=mesh, in_specs=in_specs, out_specs=P(None, "elem"), check_vma=False)
```
